32 devices in a mesh: dp: 4 (over y, x), expert: 8 (over z, core).
Axes of the slice: x: 2, y: 2, z: 4, core: 2. Of those that a mesh axis runs over, the one named last changes fastest.
Arguments:
- out_grad: bfloat16 [384, 3072], P(('dp', 'expert')), may hold values from -6 to 6
- layer_input: bfloat16 [384, 3072], P(('dp', 'expert')), may hold values from -6 to 6
- expert_ids: int32 [384, 2], P(('dp', 'expert')), may hold values from 0 to 7, as said below
- gate_prob: float32 [384, 2], P(('dp', 'expert')), may hold values from 0.05 to 1
- w_stack: bfloat16 [3, 3072, 8192], P(None, 'dp', 'expert'), may hold values from -0.109375 to 0.109375
- scale_exps: int32 [3, 24, 64], P(None, 'dp', 'expert'), may hold values from -1 to 1
Outputs:
- input_grad: bfloat16 [384, 3072], P(('dp', 'expert'))
- weight_grads: float32 [3, 3072, 8192], P(None, 'dp', 'expert')
The draws below stay inside these ranges and needn't reach their ends.
Inputs may be any that keep to these rules, and one draw needn't show every extreme that they name: `expert_ids`: each row names two different experts. In each aligned block of 12 rows (the tokens of one device) between 1 and 3 rows name expert 0, and some blocks have exactly 3 in every draw.
All inputs are finite; a program needn't handle non-finite values.
Results may differ from the reference program's by a relative error of at most 0.015.
Values may be sent and summed in bfloat16 or wider, within the bound.
A program may use at most 128 MiB of HBM per device.

```python
import math
import jax
import jax.numpy as jnp
from jax import lax

D = 3072
FF = 8192
EXPERTS = 8
TOP = 2
TILE = 128
CAP = 3
TOK_DEV = 12
TOKENS = 384
N_DP = 4
N_EXPERT = 8


def draw_expert_ids(key, part):
    block_count = TOKENS // TOK_DEV
    subkeys = jax.random.split(jax.random.fold_in(key, 11), 7)
    counts = jax.random.randint(subkeys[0], (block_count,), 1, CAP + 1)
    full_block = jax.random.randint(subkeys[1], (block_count,), 0, 4) == 0
    chosen = jax.random.randint(subkeys[2], (), 0, block_count)
    counts = jnp.where(full_block | (jnp.arange(block_count) == chosen), CAP, counts)
    ranks = jax.vmap(lambda subkey: jax.random.permutation(subkey, TOK_DEV))(jax.random.split(subkeys[3], block_count))
    routed = ranks < counts[:, None]
    first_pick = jax.random.randint(subkeys[4], (block_count, TOK_DEV), 1, EXPERTS)
    offset = jax.random.randint(subkeys[5], (block_count, TOK_DEV), 1, EXPERTS - 1)
    second = 1 + (first_pick - 1 + offset) % (EXPERTS - 1)
    flipped = jax.random.randint(subkeys[6], (block_count, TOK_DEV), 0, 2) == 1
    column_left = jnp.where(routed, jnp.where(flipped, first_pick, 0), first_pick)
    column_right = jnp.where(routed, jnp.where(flipped, 0, first_pick), second)
    return jnp.stack([column_left, column_right], axis=-1).reshape(TOKENS, 2).astype(jnp.int32)


def with_ends(entries, stream_key, low, high):
    longest = entries.shape.index(max(entries.shape))
    spots = []
    for shift in (0, 1):
        where = [jax.random.randint(jax.random.fold_in(stream_key, axis), (), 0, length) for axis, length in enumerate(entries.shape)]
        where[longest] = (where[longest] + shift) % entries.shape[longest]
        spots.append(tuple(where))
    return entries.at[spots[0]].set(low).at[spots[1]].set(high)


def levels(rng, shape, cuts, low, high):
    def one(axis_at, parts):
        steps = jax.random.uniform(jax.random.fold_in(jax.random.fold_in(rng, 6), axis_at), (parts,), jnp.float32, low / len(cuts), high / len(cuts))
        return jnp.repeat(jnp.exp(steps), shape[axis_at] // parts).reshape((-1,) + (1,) * (len(shape) - axis_at - 1))

    loudness = one(*cuts[0])
    for cut in cuts[1:]:
        loudness = loudness * one(*cut)
    return loudness


def scatter_about(stream_key, dims, deviation, limit, pieces=(), kind=jnp.bfloat16):
    drawn = jax.random.normal(stream_key, dims, jnp.float32) * deviation
    if len(pieces) > 0:
        drawn = levels(stream_key, dims, pieces, -0.22, 0.18) * drawn
    return jnp.clip(drawn, min=-limit, max=limit).astype(kind)


def setup_inputs(seed: int = 0) -> dict:
    key_list = jax.random.split(jax.random.key(seed), 7)
    return {
        "out_grad": scatter_about(key_list[0], (TOKENS, D), 1.0, 6.0, ((0, 32),)),
        "layer_input": scatter_about(key_list[1], (TOKENS, D), 1.0, 6.0, ((0, 32),)),
        "expert_ids": draw_expert_ids(jax.random.fold_in(key_list[6], 71), 0),
        "gate_prob": jnp.clip(jnp.exp(math.log(1.0) - 2.9957323 * jax.random.uniform(key_list[3], (TOKENS, TOP), jnp.float32) ** levels(key_list[3], (TOKENS, TOP), ((0, 32),), -0.2, 0.2)), 0.05, 1.0),
        "w_stack": scatter_about(key_list[4], (3, D, FF), D ** -0.5, 0.109375, ((1, 4), (2, 8))),
        "scale_exps": with_ends(jax.random.randint(key_list[5], (3, D // TILE, FF // TILE), -1, 2), jax.random.fold_in(key_list[5], 1), -1, 1).astype(jnp.int32),
    }


def dequantize(w_stack, scale_exps):
    factor = jnp.exp2(scale_exps.astype(jnp.float32))
    scaled = w_stack.astype(jnp.float32).reshape(3, D // TILE, TILE, FF // TILE, TILE) * factor[:, :, None, :, None]
    return scaled.reshape(3, D, FF).astype(jnp.bfloat16)


def contract_rows(left, right):
    return lax.dot_general(left, right, (((0,), (0,)), ((), ())), preferred_element_type=jnp.float32)


def back_project(grad_rows, matrix):
    return lax.dot_general(grad_rows, matrix, (((1,), (1,)), ((), ())), preferred_element_type=jnp.float32)


def expert_backward(routed_input, routed_grad, weights):
    gate_value = jnp.dot(routed_input, weights[0], preferred_element_type=jnp.float32)
    up_value = jnp.dot(routed_input, weights[1], preferred_element_type=jnp.float32)
    down_back = jnp.dot(routed_grad, weights[2], preferred_element_type=jnp.float32)
    gate_sigmoid = jax.nn.sigmoid(gate_value)
    gate_act = gate_value * gate_sigmoid
    gate_grad = (down_back * up_value * gate_sigmoid * (1.0 + gate_value * (1.0 - gate_sigmoid))).astype(jnp.bfloat16)
    up_grad = (down_back * gate_act).astype(jnp.bfloat16)
    hidden = (gate_act * up_value).astype(jnp.bfloat16)
    returned = back_project(gate_grad, weights[0]) + back_project(up_grad, weights[1])
    partial_value = jnp.stack([contract_rows(routed_input, gate_grad), contract_rows(routed_input, up_grad), contract_rows(routed_grad, hidden)])
    return returned, partial_value


def reference(out_grad, layer_input, expert_ids, gate_prob, w_stack, scale_exps):
    weights = dequantize(w_stack, scale_exps)
    routed = expert_ids == 0
    routed_mask = jnp.any(routed, axis=1)
    expert_prob = jnp.sum(jnp.where(routed, gate_prob, 0.0), axis=1)
    block_count = out_grad.shape[0] // TOK_DEV
    block_mask = routed_mask.reshape(block_count, TOK_DEV)
    slot_index = jnp.cumsum(block_mask.astype(jnp.int32), axis=1) - 1
    places = jnp.arange(CAP, dtype=jnp.int32)
    slot_hit = (slot_index[:, None, :] == places[None, :, None]) & block_mask[:, None, :]
    positions = jnp.arange(TOK_DEV, dtype=jnp.int32)
    source = jnp.sum(jnp.where(slot_hit, positions[None, None, :], 0), axis=2)
    source = (source + (jnp.arange(block_count, dtype=jnp.int32) * TOK_DEV)[:, None]).reshape(-1)
    slot_valid = jnp.any(slot_hit, axis=2).reshape(-1)
    slot_input = jnp.where(slot_valid[:, None], layer_input[source], jnp.zeros((), jnp.bfloat16))
    slot_grad = jnp.where(slot_valid[:, None], expert_prob[source][:, None] * out_grad[source].astype(jnp.float32), 0.0).astype(jnp.bfloat16)
    slot_rows = N_EXPERT * CAP
    group_input = slot_input.reshape(N_DP, slot_rows, D)
    group_grad = slot_grad.reshape(N_DP, slot_rows, D)

    def group_step(total, pair):
        returned, partial_value = expert_backward(pair[0], pair[1], weights)
        rounded = lax.optimization_barrier(partial_value.astype(jnp.bfloat16))
        return total + rounded.astype(jnp.float32), returned

    weight_grads, returned = lax.scan(group_step, jnp.zeros((3, D, FF), jnp.float32), (group_input, group_grad))
    returned = returned.reshape(block_count, CAP, D)
    picked = jnp.take_along_axis(returned, jnp.clip(slot_index, 0, CAP - 1)[:, :, None], axis=1)
    input_grad = jnp.where(block_mask[:, :, None], picked, 0.0).reshape(-1, D).astype(jnp.bfloat16)
    return input_grad, weight_grads
```

```python
import functools

import jax
import jax.numpy as jnp
from jax import lax
from jax.experimental import pallas as pl
from jax.experimental.pallas import tpu as pltpu
from jax.sharding import PartitionSpec as P

TILE = 128
CAP = 3
DIRECT = 64
TALL = 256
BF = jnp.bfloat16
F32 = jnp.float32
VMEM_LIMIT = 40 * 1024 * 1024


def iota(shape, dim):
    return lax.broadcasted_iota(jnp.int32, shape, dim)


def mm(a, b, ca=1, cb=0):
    return lax.dot_general(a, b, (((ca,), (cb,)), ((), ())), preferred_element_type=F32)


def exchange_kernel(
    n_dp, n_ex, chunk,
    og_hbm, li_hbm, ids_hbm, prob_hbm, exps_hbm, w_hbm,
    wg_ref, ig_ref,
    og_ref, li_ref, ids_ref, prob_ref, exps_ref, xt, act, w, slab_out, slabs, x, part_out, part_in, acts, hids, acc, back_out, back_in, own_out, own_in,
    in_sem, w_sem, s1_send, s1_recv, s2_send, s2_recv, s3_send, s3_recv, rs_send, rs_recv,
    ag_send, ag_recv, hg_send, hg_recv, b1_send, b1_recv, b2_send, b2_recv,
):
    p, e = lax.axis_index("dp"), lax.axis_index("expert")
    tok, width = og_hbm.shape
    _, depth, hid = w.shape
    rows = n_ex * CAP
    n_chunk = hid // chunk
    pairs = n_ex // 2
    z, core = e // 2, e % 2
    partner = 2 * z + 1 - core

    def send(src, dst, ssem, rsem, q, f):
        copy = pltpu.make_async_remote_copy(
            src_ref=src, dst_ref=dst, send_sem=ssem, recv_sem=rsem,
            device_id=(q, f), device_id_type=pl.DeviceIdType.MESH,
        )
        copy.start()
        return copy

    barrier = pltpu.get_barrier_semaphore()
    for k in range(1, n_dp):
        pl.semaphore_signal(
            barrier, inc=1, device_id=(lax.rem(p + k, n_dp), e),
            device_id_type=pl.DeviceIdType.MESH,
        )
    for k in range(1, n_ex):
        pl.semaphore_signal(
            barrier, inc=1, device_id=(p, lax.rem(e + k, n_ex)),
            device_id_type=pl.DeviceIdType.MESH,
        )

    in_copies = [
        pltpu.make_async_copy(src, dst, in_sem.at[i])
        for i, (src, dst) in enumerate((
            (ids_hbm, ids_ref), (prob_hbm, prob_ref), (li_hbm, li_ref),
            (og_hbm, og_ref), (exps_hbm, exps_ref),
        ))
    ]
    for copy in in_copies:
        copy.start()
    w_copies = [
        pltpu.make_async_copy(w_hbm.at[m], w.at[m], w_sem.at[m]) for m in range(3)
    ]
    for copy in w_copies:
        copy.start()

    for copy in in_copies[:4]:
        copy.wait()
    routed = ids_ref[...] == 0
    mask = jnp.max(routed.astype(F32), axis=0, keepdims=True)
    prob = jnp.sum(jnp.where(routed, prob_ref[...], 0.0), axis=0, keepdims=True)
    earlier = (iota((tok, tok), 0) <= iota((tok, tok), 1)).astype(BF)
    place = mm(jnp.broadcast_to(mask, (8, tok)).astype(BF), earlier) - 1.0
    mask_tall = jnp.broadcast_to(mask, (8, tok)) > 0.5
    row = iota((8, tok), 0).astype(F32)
    hit_in = jnp.where((place == row) & (row < CAP) & mask_tall, 1.0, 0.0)
    hit_gr = jnp.where((place + CAP == row) & (row >= CAP) & mask_tall, 1.0, 0.0)
    row_prob = jnp.sum(hit_gr * prob, axis=1, keepdims=True)
    slots = (
        mm(hit_in.astype(BF), li_ref[...]) + row_prob * mm(hit_gr.astype(BF), og_ref[...])
    ).astype(BF)
    for q in range(n_dp):
        slab_out[q] = slots[:, q * depth:(q + 1) * depth]
    pl.semaphore_wait(barrier, n_dp - 1 + n_ex - 1)

    pend = []
    for k in range(1, n_dp):
        q = lax.rem(p + k, n_dp)
        pend.append(send(slab_out.at[q], slabs.at[e, p], s1_send.at[k], s1_recv.at[k], q, e))
    slabs[e, p] = slab_out[p]
    for copy in pend:
        copy.wait()

    pend = [send(slabs.at[e], slabs.at[e], s2_send.at[0], s2_recv.at[0], p, partner)]
    for k in range(1, pairs):
        f = 2 * lax.rem(z + k, pairs) + core
        pend.append(send(slabs.at[e], slabs.at[e], s2_send.at[k], s2_recv.at[k], p, f))

    in_copies[4].wait()
    for copy in w_copies:
        copy.wait()
    tr, tc = depth // TILE, hid // TILE

    def scale_rows(i, carry):
        m, r = i // tr, i % tr
        at = pl.ds(pl.multiple_of(r * TILE, TILE), TILE)
        for j in range(tc):
            power = lax.shift_left(jnp.int32(1), exps_ref[m, r, j] + 15)
            factor = power.astype(F32) * (2.0 ** -15)
            cols = slice(j * TILE, (j + 1) * TILE)
            w[m, at, cols] = (w[m, at, cols].astype(F32) * factor).astype(BF)
        return carry

    lax.fori_loop(0, 3 * tr, scale_rows, 0)

    relays = []
    for k in range(1, pairs):
        pend[k].wait_recv()
        f = 2 * lax.rem(z - k + pairs, pairs) + core
        relays.append(send(slabs.at[f], slabs.at[f], s3_send.at[k], s3_recv.at[k], p, partner))
    pend[0].wait_recv()
    for copy in relays:
        copy.wait_recv()

    src, dst = iota((2 * rows, n_ex * 8), 1), iota((2 * rows, n_ex * 8), 0)
    kind, rest = dst // rows, dst % rows
    pick = jnp.where(
        src == (rest // CAP) * 8 + kind * CAP + rest % CAP, 1.0, 0.0
    ).astype(BF)
    got = [mm(pick, slabs[:, g].reshape(n_ex * 8, depth)) for g in range(n_dp)]
    xs = [
        jnp.concatenate([v[i * rows:(i + 1) * rows] for v in got], axis=0) for i in range(2)
    ]
    for i in range(2):
        x[i] = xs[i].astype(BF)

    sent = []
    for c in range(n_chunk):
        cols = slice(c * chunk, (c + 1) * chunk)
        for m in range(3):
            val = mm(x[m // 2], w[m, :, cols]).astype(F32)
            for g in range(n_dp):
                part_out[c, g, m] = val[g * rows:(g + 1) * rows].astype(BF)
        line = []
        for k in range(1, n_dp):
            q = lax.rem(p + k, n_dp)
            line.append(send(
                part_out.at[c, q], part_in.at[c, k], rs_send.at[c, k], rs_recv.at[c, k], q, e
            ))
        sent.append(line)

    for i in range(2):
        xt[i] = x[i].astype(F32).T.astype(BF)

    shared = []
    for c in range(n_chunk):
        total = [part_out[c, p, m].astype(F32) for m in range(3)]
        for k in range(1, n_dp):
            sent[c][k - 1].wait_recv()
            total = [total[m] + part_in[c, k, m].astype(F32) for m in range(3)]
        gate, up, down = total
        sig = jax.nn.sigmoid(gate)
        silu = gate * sig
        acts[c, p, 0] = (down * up * sig * (1.0 + gate * (1.0 - sig))).astype(BF)
        acts[c, p, 1] = (down * silu).astype(BF)
        hids[c, p] = (silu * up).astype(BF)
        line = []
        for k in range(1, n_dp):
            q = lax.rem(p + k, n_dp)
            line.append(send(
                acts.at[c, p], acts.at[c, p], ag_send.at[c, k], ag_recv.at[c, k], q, e
            ))
        shared.append(line)

    late = []
    for c in range(n_chunk):
        for k in range(1, n_dp):
            q = lax.rem(p + k, n_dp)
            late.append(send(
                hids.at[c, p], hids.at[c, p], hg_send.at[c, k], hg_recv.at[c, k], q, e
            ))

    for c in range(n_chunk):
        cols = slice(c * chunk, (c + 1) * chunk)
        for copy in shared[c]:
            copy.wait_recv()
        full = []
        for m in range(2):
            val = jnp.concatenate(
                [acts[c, g, m].astype(F32) for g in range(n_dp)], axis=0
            ).astype(BF)
            act[m, :, cols] = val
            full.append(val)
        part = mm(full[0], w[0, :, cols], 1, 1) + mm(full[1], w[1, :, cols], 1, 1)
        if c == 0:
            acc[...] = part
        else:
            acc[...] += part

    pad = n_dp * 2
    half = depth // 2
    summed = acc[...].astype(BF)
    batch = min(n_ex, 8)
    for b in range(n_ex // batch):
        shape = (batch * pad, n_dp * rows)
        to, frm = iota(shape, 0), iota(shape, 1)
        f, g = to // pad + b * batch, (to % pad) // 2
        parts = []
        for t in range(CAP):
            piece = CAP * (to % 2) + t
            val = 0.0
            for h in range(2):
                choose = jnp.where(
                    (piece % 2 == h) & (frm == g * rows + f * CAP + piece // 2), 1.0, 0.0
                ).astype(BF)
                val = val + mm(choose, summed[:, h * half:(h + 1) * half])
            parts.append(val)
        val = jnp.concatenate(parts, axis=1)
        for j in range(batch):
            for g in range(n_dp):
                at = j * pad + g * 2
                back_out[b * batch + j, g] = val[at:at + 2].astype(BF)
    tall = min(TALL, depth)

    def weight_grads():
        for m in range(3):
            if m == 2:
                for copy in late:
                    copy.wait_recv()
                for c in range(n_chunk):
                    act[2, :, c * chunk:(c + 1) * chunk] = jnp.concatenate(
                        [hids[c, g].astype(F32) for g in range(n_dp)], axis=0
                    ).astype(BF)
            for r in range(0, depth, tall):
                at = slice(r, r + tall)
                wg_ref[m, at, :] = mm(xt[m // 2, at, :], act[m])

    back, last = [], []
    if n_dp * n_ex <= DIRECT:
        for kf in range(n_ex - 1, -1, -1):
            for kq in range(n_dp - 1, -1, -1):
                if kq or kf:
                    q, f = lax.rem(p + kq, n_dp), lax.rem(e + kf, n_ex)
                    back.append(send(
                        back_out.at[f, q], back_in.at[e, p],
                        b1_send.at[kf, kq], b1_recv.at[kf, kq], q, f,
                    ))
        back_in[e, p] = back_out[e, p]
        weight_grads()
        for copy in back:
            copy.wait_recv()
        for q in range(n_dp):
            total = back_in[0, q].astype(F32)
            for f in range(1, n_ex):
                total = total + back_in[f, q].astype(F32)
            own_in[q] = total.astype(BF)
    else:
        for k in range(1, n_ex):
            f = lax.rem(e + k, n_ex)
            back.append(send(back_out.at[f], back_in.at[k], b1_send.at[k, 0], b1_recv.at[k, 0], p, f))
        weight_grads()
        total = [back_out[e, g].astype(F32) for g in range(n_dp)]
        for k in range(1, n_ex):
            back[k - 1].wait_recv()
            total = [total[g] + back_in[k, g].astype(F32) for g in range(n_dp)]
        for g in range(n_dp):
            own_out[g] = total[g].astype(BF)
        for k in range(1, n_dp):
            q = lax.rem(p + k, n_dp)
            last.append(send(own_out.at[q], own_in.at[p], b2_send.at[k], b2_recv.at[k], q, e))
        own_in[p] = own_out[p]
        for copy in last:
            copy.wait_recv()
    for q in range(n_dp):
        packed = own_in[q].astype(F32)
        halves = [
            packed[j // CAP:j // CAP + 1, (j % CAP) * half:(j % CAP + 1) * half]
            for j in range(2 * CAP)
        ]
        back_rows = jnp.concatenate(
            [jnp.concatenate(halves[2 * c:2 * c + 2], axis=1) for c in range(CAP)], axis=0
        ).astype(BF)
        ig_ref[:, q * depth:(q + 1) * depth] = mm(
            hit_in[:CAP].astype(BF), back_rows, 0, 0
        ).astype(BF)

    for copy in pend[:pairs] + relays + late + back + last:
        copy.wait_send()
    for line in sent + shared:
        for copy in line:
            copy.wait_send()


def store_kernel(wg_ref, ig_ref, wg_hbm, ig_hbm, sems):
    copies = [pltpu.make_async_copy(ig_ref, ig_hbm, sems.at[3])]
    for m in range(3):
        copies.append(pltpu.make_async_copy(wg_ref.at[m], wg_hbm.at[m], sems.at[m]))
    for copy in copies:
        copy.start()
    for copy in copies:
        copy.wait()


def per_device(n_dp, n_ex, out_grad, layer_input, expert_ids, gate_prob, w_stack, scale_exps):
    tok, width = out_grad.shape
    _, depth, hid = w_stack.shape
    rows = n_ex * CAP
    total = n_dp * rows
    chunk = min(256, hid)
    n_chunk = hid // chunk
    n_last = n_dp if n_dp * n_ex <= DIRECT else 1
    vm = pl.BlockSpec(memory_space=pltpu.VMEM)
    dma = pltpu.SemaphoreType.DMA
    pairs = n_ex // 2
    weight_grads, input_grad = pl.pallas_call(
        functools.partial(exchange_kernel, n_dp, n_ex, chunk),
        out_shape=(
            jax.ShapeDtypeStruct((3, depth, hid), F32),
            jax.ShapeDtypeStruct((tok, width), BF),
        ),
        in_specs=[pl.BlockSpec(memory_space=pltpu.HBM)] * 6,
        out_specs=(vm, vm),
        scratch_shapes=[
            pltpu.VMEM((tok, width), BF),
            pltpu.VMEM((tok, width), BF),
            pltpu.VMEM((2, tok), jnp.int32),
            pltpu.VMEM((2, tok), F32),
            pltpu.SMEM(scale_exps.shape, jnp.int32),
            pltpu.VMEM((2, depth, total), BF),
            pltpu.VMEM((3, total, hid), BF),
            pltpu.VMEM((3, depth, hid), BF),
            pltpu.VMEM((n_dp, 8, depth), BF),
            pltpu.VMEM((n_ex, n_dp, 8, depth), BF),
            pltpu.VMEM((2, total, depth), BF),
            pltpu.VMEM((n_chunk, n_dp, 3, rows, chunk), BF),
            pltpu.VMEM((n_chunk, n_dp, 3, rows, chunk), BF),
            pltpu.VMEM((n_chunk, n_dp, 2, rows, chunk), BF),
            pltpu.VMEM((n_chunk, n_dp, rows, chunk), BF),
            pltpu.VMEM((total, depth), F32),
            pltpu.VMEM((n_ex, n_dp, 2, CAP * depth // 2), BF),
            pltpu.VMEM((n_ex, n_dp, 2, CAP * depth // 2), BF),
            pltpu.VMEM((n_dp, 2, CAP * depth // 2), BF),
            pltpu.VMEM((n_dp, 2, CAP * depth // 2), BF),
            dma((5,)), dma((3,)),
            dma((n_dp,)), dma((n_dp,)),
            dma((pairs,)), dma((pairs,)),
            dma((pairs,)), dma((pairs,)),
            dma((n_chunk, n_dp)), dma((n_chunk, n_dp)),
            dma((n_chunk, n_dp)), dma((n_chunk, n_dp)),
            dma((n_chunk, n_dp)), dma((n_chunk, n_dp)),
            dma((n_ex, n_last)), dma((n_ex, n_last)),
            dma((n_dp,)), dma((n_dp,)),
        ],
        compiler_params=pltpu.CompilerParams(
            collective_id=0, has_side_effects=True, vmem_limit_bytes=VMEM_LIMIT
        ),
    )(*(
        pltpu.with_memory_space_constraint(v, pltpu.HBM)
        for v in (out_grad, layer_input, expert_ids.T, gate_prob.T, scale_exps, w_stack)
    ))
    weight_grads, input_grad = pl.pallas_call(
        store_kernel,
        in_specs=[vm, vm],
        out_specs=(pl.BlockSpec(memory_space=pl.ANY), pl.BlockSpec(memory_space=pl.ANY)),
        out_shape=(
            jax.ShapeDtypeStruct((3, depth, hid), F32),
            jax.ShapeDtypeStruct((tok, width), BF),
        ),
        scratch_shapes=[dma((4,))],
        compiler_params=pltpu.CompilerParams(vmem_limit_bytes=VMEM_LIMIT),
    )(weight_grads, input_grad)
    return input_grad, weight_grads


def solution(mesh):
    in_specs = (
        P(("dp", "expert"), None),
        P(("dp", "expert"), None),
        P(("dp", "expert"), None),
        P(("dp", "expert"), None),
        P(None, "dp", "expert"),
        P(None, "dp", "expert"),
    )
    out_specs = (P(("dp", "expert"), None), P(None, "dp", "expert"))
    return jax.shard_map(
        functools.partial(per_device, mesh.shape["dp"], mesh.shape["expert"]),
        mesh=mesh, in_specs=in_specs, out_specs=out_specs, check_vma=False,
    )
```

```python
import functools

import jax
import jax.numpy as jnp
from jax import lax
from jax.experimental import pallas as pl
from jax.experimental.pallas import tpu as pltpu
from jax.sharding import PartitionSpec as P

TILE = 128
CAP = 3
DIRECT = 64
TALL = 256
BF = jnp.bfloat16
F32 = jnp.float32
VMEM_LIMIT = 40 * 1024 * 1024


def iota(shape, dim):
    return lax.broadcasted_iota(jnp.int32, shape, dim)


def mm(a, b, ca=1, cb=0):
    return lax.dot_general(a, b, (((ca,), (cb,)), ((), ())), preferred_element_type=F32)


def up8(n):
    return -(-n // 8) * 8


def step_to(i, k, n):
    return i ^ k if n & (n - 1) == 0 else lax.rem(i + k, n)


def step_from(i, k, n):
    return i ^ k if n & (n - 1) == 0 else lax.rem(i - k + n, n)


def pad_rows(val, n):
    if val.shape[0] == n:
        return val
    return jnp.concatenate([val, jnp.zeros((n - val.shape[0], val.shape[1]), val.dtype)], axis=0)


class Batch:
    def __init__(self, steps, first, last, n_dp, hid):
        self.steps = steps
        self.rows = len(steps) * 2 * CAP
        self.padded = up8(self.rows)
        tight = up8(3 * self.rows) < 3 * self.padded
        self.stride = self.rows if tight else self.padded
        self.first = first
        self.last = last
        self.all = n_dp * self.padded
        self.mats = 2 if last else 3
        self.sum_rows = up8(3 * self.stride)
        self.act_rows = up8(self.mats * self.stride)
        self.chunk = min(256 if last else 512, hid)
        self.n_chunk = hid // self.chunk

    def cols(self, c):
        return slice(c * self.chunk, (c + 1) * self.chunk)


def plan_batches(n_dp, n_ex, hid):
    pairs = n_ex // 2
    groups = [[0], [1], list(range(2, pairs))] if 2 < pairs <= 4 else [list(range(pairs))]
    batches, first = [], 0
    for i, steps in enumerate(groups):
        batches.append(Batch(steps, first, i == len(groups) - 1, n_dp, hid))
        first += batches[-1].all
    return batches


def exchange_kernel(
    n_dp, n_ex, batches,
    og_hbm, li_hbm, ids_hbm, prob_hbm, exps_hbm, w_hbm,
    wg_ref, ig_ref, *scratch,
):
    n_b = len(batches)
    (
        og_ref, li_ref, ids_ref, prob_ref, exps_ref, xt, act, w, slab_out, slabs, x, hid_out, hid_in,
        acc, back_out, back_in, own_out, own_in,
        in_sem, s1_send, s1_recv, s2_send, s2_recv, s3_send, s3_recv, ready,
        rs_send, rs_recv, ag_send, ag_recv, hg_sem, b1_sem, b2_sem,
    ) = scratch[:33]
    bufs = scratch[33:]
    part_out, part_in, act_out, act_in = (bufs[i * n_b:(i + 1) * n_b] for i in range(4))
    p, e = lax.axis_index("dp"), lax.axis_index("expert")
    tok, width = og_hbm.shape
    _, depth, hid = w.shape
    pairs = n_ex // 2
    z, core = e // 2, e % 2
    other = 1 - core
    partner = 2 * z + other

    def send(src, dst, ssem, rsem, q, f):
        pltpu.make_async_remote_copy(
            src_ref=src, dst_ref=dst, send_sem=ssem, recv_sem=rsem,
            device_id=(q, f), device_id_type=pl.DeviceIdType.MESH,
        ).start()

    def wait(ref, sem):
        pltpu.make_async_copy(ref, ref, sem).wait()

    def tell(sem, q, f):
        pl.semaphore_signal(sem, inc=1, device_id=(q, f), device_id_type=pl.DeviceIdType.MESH)

    in_copies = [
        pltpu.make_async_copy(src, dst, in_sem.at[i])
        for i, (src, dst) in enumerate((
            (ids_hbm, ids_ref), (prob_hbm, prob_ref), (li_hbm, li_ref),
            (og_hbm, og_ref), (exps_hbm, exps_ref), (w_hbm, w),
        ))
    ]
    for copy in in_copies[:5]:
        copy.start()

    barrier = pltpu.get_barrier_semaphore()
    for k in range(1, n_dp):
        tell(barrier, step_from(p, k, n_dp), partner)
    tell(barrier, p, partner)
    for j in range(1, pairs):
        s = step_from(z, j, pairs)

        @pl.when(s > z)
        def _(s=s):
            tell(barrier, p, 2 * s + other)

    for copy in in_copies[:4]:
        copy.wait()
    in_copies[5].start()
    routed = ids_ref[...] == 0
    mask = jnp.max(routed.astype(F32), axis=0, keepdims=True)
    prob = jnp.sum(jnp.where(routed, prob_ref[...], 0.0), axis=0, keepdims=True)
    earlier = (iota((tok, tok), 0) <= iota((tok, tok), 1)).astype(BF)
    place = mm(jnp.broadcast_to(mask, (8, tok)).astype(BF), earlier) - 1.0
    mask_tall = jnp.broadcast_to(mask, (8, tok)) > 0.5
    row = iota((8, tok), 0).astype(F32)
    hit_in = jnp.where((place == row) & (row < CAP) & mask_tall, 1.0, 0.0)
    hit_gr = jnp.where((place + CAP == row) & (row >= CAP) & mask_tall, 1.0, 0.0)
    row_prob = jnp.sum(hit_gr * prob, axis=1, keepdims=True)
    slots = (
        mm(hit_in.astype(BF), li_ref[...]) + row_prob * mm(hit_gr.astype(BF), og_ref[...])
    ).astype(BF)
    for q in range(n_dp):
        slab_out[q] = slots[:, q * depth:(q + 1) * depth]
    pl.semaphore_wait(barrier, n_dp + z)

    for k in range(n_dp - 1, 0, -1):
        q = step_to(p, k, n_dp)
        send(slab_out.at[q], slabs.at[z, other, p], s1_send, s1_recv.at[k], q, partner)
    for j in range(1, pairs):
        s = step_from(z, j, pairs)

        @pl.when(s < z)
        def _(s=s, j=j):
            tell(ready.at[j], p, 2 * s + other)

    slabs[z, core, p] = slab_out[p]

    def forward_down(src):
        for j in range(pairs - 1, 0, -1):
            t = step_to(z, j, pairs)

            @pl.when(t < z)
            def _(t=t, j=j):
                send(src, src, s2_send, s2_recv.at[j], p, 2 * t + other)

    fine = n_dp <= 4
    if fine:
        forward_down(slabs.at[z, core, p])

    in_copies[4].wait()
    in_copies[5].wait()
    tr, tc = depth // TILE, hid // TILE

    def scale_rows(i, carry):
        m, r = i // tr, i % tr
        at = pl.ds(pl.multiple_of(r * TILE, TILE), TILE)
        for j in range(tc):
            power = lax.shift_left(jnp.int32(1), exps_ref[m, r, j] + 15)
            factor = power.astype(F32) * (2.0 ** -15)
            cols = slice(j * TILE, (j + 1) * TILE)
            w[m, at, cols] = (w[m, at, cols].astype(F32) * factor).astype(BF)
        return carry

    lax.fori_loop(0, 3 * tr, scale_rows, 0)

    for k in range(1, n_dp):
        q = step_from(p, k, n_dp)
        wait(slabs.at[z, core, q], s1_recv.at[k])
        if fine:
            forward_down(slabs.at[z, core, q])
    held = slabs.at[z, core]
    send(held, held, s3_send, s3_recv.at[0], p, partner)
    if not fine:
        forward_down(held)
    for j in range(1, pairs):
        t = step_to(z, j, pairs)

        @pl.when(t > z)
        def _(t=t, j=j):
            pl.semaphore_wait(ready.at[j], 1)
            send(held, held, s2_send, s2_recv.at[j], p, 2 * t + other)

    def pass_on(b):
        for j in b.steps:
            if j:
                block = slabs.at[step_from(z, j, pairs), other]
                wait(block, s2_recv.at[j])
                send(block, block, s3_send, s3_recv.at[j], p, partner)

    def collect(b):
        for j in b.steps:
            s = step_from(z, j, pairs)
            wait(slabs.at[s, core if j else other], s3_recv.at[j])
        shape = (2 * b.padded, len(b.steps) * 16)
        src, dst = iota(shape, 1), iota(shape, 0)
        kind, r = dst // b.padded, dst % b.padded
        jl, cs, c = r // (2 * CAP), (r // CAP) % 2, r % CAP
        rows = [[], []]
        for g in range(n_dp):
            h = jnp.where(g == p, cs, 1 - cs)
            pick = jnp.where(
                (src == jl * 16 + h * 8 + kind * CAP + c) & (r < b.rows), 1.0, 0.0
            ).astype(BF)
            have = jnp.concatenate(
                [slabs[step_from(z, j, pairs), :, g].reshape(16, depth) for j in b.steps], axis=0
            )
            val = mm(pick, have)
            for i in range(2):
                rows[i].append(val[i * b.padded:(i + 1) * b.padded])
        for i in range(2):
            x[i, b.first:b.first + b.all] = jnp.concatenate(rows[i], axis=0).astype(BF)

    def multiply(n, c):
        b = batches[n]
        vals = [
            mm(x[m // 2, b.first:b.first + b.all], w[m, :, b.cols(c)]) for m in range(3)
        ]
        for g in range(n_dp):
            at = g * b.padded
            block = jnp.concatenate([v[at:at + b.stride] for v in vals], axis=0)
            part_out[n][c, g] = pad_rows(block, b.sum_rows).astype(BF)
        for k in range(n_dp - 1, -1, -1):
            q = step_to(p, k, n_dp)
            send(part_out[n].at[c, q], part_in[n].at[c, p], rs_send.at[n], rs_recv.at[n, c], q, partner)

    pass_on(batches[0])
    for n, b in enumerate(batches):
        collect(b)
        for c in range(b.n_chunk):
            if c == b.n_chunk - 1 and not b.last:
                if c == 0 or n > 0:
                    pass_on(batches[n + 1])
            multiply(n, c)
        if n == 0 and b.n_chunk > 1 and not b.last:
            pass_on(batches[1])

    for i in range(2):
        xt[i] = x[i].astype(F32).T.astype(BF)

    for n, b in enumerate(batches):
        for c in range(b.n_chunk):
            wait(part_in[n].at[c], rs_recv.at[n, c])
            total = part_in[n][c, 0].astype(F32)
            for g in range(1, n_dp):
                total = total + part_in[n][c, g].astype(F32)
            gate, up, down = (total[m * b.stride:(m + 1) * b.stride] for m in range(3))
            sig = jax.nn.sigmoid(gate)
            silu = gate * sig
            grads = [down * up * sig * (1.0 + gate * (1.0 - sig)), down * silu]
            hidden = silu * up
            if b.last:
                hid_out[:, b.cols(c)] = pad_rows(hidden, b.padded).astype(BF)
            else:
                grads.append(hidden)
            act_out[n][c] = pad_rows(jnp.concatenate(grads, axis=0), b.act_rows).astype(BF)
            for k in range(n_dp - 1, -1, -1):
                q = step_to(p, k, n_dp)
                send(act_out[n].at[c], act_in[n].at[c, p], ag_send.at[n], ag_recv.at[n, c], q, partner)
    for k in range(n_dp - 1, -1, -1):
        send(hid_out, hid_in.at[p], hg_sem.at[0], hg_sem.at[1], step_to(p, k, n_dp), partner)

    def unpack(n, c):
        b = batches[n]
        wait(act_in[n].at[c], ag_recv.at[n, c])
        blocks = [act_in[n][c, g].astype(F32) for g in range(n_dp)]
        for m in range(b.mats):
            val = [pad_rows(v[m * b.stride:(m + 1) * b.stride], b.padded) for v in blocks]
            act[m, b.first:b.first + b.all, b.cols(c)] = jnp.concatenate(val, axis=0).astype(BF)

    for n, b in enumerate(batches):
        for c in range(b.n_chunk):
            unpack(n, c)
            if b.last:
                cols = b.cols(c)
                part = mm(act[0, :, cols], w[0, :, cols], 1, 1) + mm(act[1, :, cols], w[1, :, cols], 1, 1)
                if c == 0:
                    acc[...] = part
                else:
                    acc[...] += part

    pad = n_dp * 2
    half = depth // 2
    summed = acc[...].astype(BF)
    some = min(n_ex, 8)
    for i in range(n_ex // some):
        shape = (some * pad, summed.shape[0])
        to, frm = iota(shape, 0), iota(shape, 1)
        f, g = to // pad + i * some, (to % pad) // 2
        cs = jnp.where(core == 0, f % 2, 1 - f % 2)
        if n_b == 1:
            base = g * batches[0].padded + (f // 2) * 2 * CAP
        else:
            base = 0
            for b in batches:
                for jl, j in enumerate(b.steps):
                    base = jnp.where(f // 2 == j, b.first + g * b.padded + jl * 2 * CAP, base)
        base = base + cs * CAP
        parts = []
        for t in range(CAP):
            piece = CAP * (to % 2) + t
            val = 0.0
            for h in range(2):
                choose = jnp.where(
                    (piece % 2 == h) & (frm == base + piece // 2), 1.0, 0.0
                ).astype(BF)
                val = val + mm(choose, summed[:, h * half:(h + 1) * half])
            parts.append(val)
        val = jnp.concatenate(parts, axis=1)
        for j in range(some):
            for g in range(n_dp):
                at = j * pad + g * 2
                back_out[i * some + j, g] = val[at:at + 2].astype(BF)

    tall = min(TALL, depth)

    def weight_grads():
        for m in range(3):
            if m == 2:
                b = batches[-1]
                wait(hid_in, hg_sem.at[1])
                act[2, b.first:b.first + b.all] = jnp.concatenate(
                    [hid_in[g].astype(F32) for g in range(n_dp)], axis=0
                ).astype(BF)
            for r in range(0, depth, tall):
                at = slice(r, r + tall)
                wg_ref[m, at, :] = mm(xt[m // 2, at, :], act[m])

    def place(q, packed):
        halves = [
            packed[j // CAP:j // CAP + 1, (j % CAP) * half:(j % CAP + 1) * half]
            for j in range(2 * CAP)
        ]
        back_rows = jnp.concatenate(
            [jnp.concatenate(halves[2 * c:2 * c + 2], axis=1) for c in range(CAP)], axis=0
        ).astype(BF)
        ig_ref[:, pl.ds(pl.multiple_of(q * depth, TILE), depth)] = mm(
            hit_in[:CAP].astype(BF), back_rows, 0, 0
        ).astype(BF)

    def far(k):
        return 2 * step_to(z, k // 2, pairs) + (core ^ (k % 2))

    if n_dp * n_ex <= DIRECT:
        for r in range(n_ex * n_dp - 1, 0, -1):
            q = step_to(p, r % n_dp, n_dp)
            send(
                back_out.at[r // n_dp, q], back_in.at[r], b1_sem.at[0], b1_sem.at[1],
                q, far(r // n_dp),
            )
        back_in[0] = back_out[0, p]
        weight_grads()
        arrived = back_in.at[1:n_ex * n_dp]
        wait(arrived, b1_sem.at[1])
        for k in range(n_dp):
            total = back_in[k].astype(F32)
            for f in range(1, n_ex):
                total = total + back_in[f * n_dp + k].astype(F32)
            place(step_from(p, k, n_dp), total)
        wait(arrived, b1_sem.at[0])
    else:
        for k in range(1, n_ex):
            send(back_out.at[k], back_in.at[k], b1_sem.at[0], b1_sem.at[1], p, far(k))
        weight_grads()
        arrived = back_in.at[1:n_ex]
        wait(arrived, b1_sem.at[1])
        for g in range(n_dp):
            total = back_out[0, g].astype(F32)
            for k in range(1, n_ex):
                total = total + back_in[k, g].astype(F32)
            own_out[g] = total.astype(BF)
        for k in range(1, n_dp):
            q = step_to(p, k, n_dp)
            send(own_out.at[q], own_in.at[k], b2_sem.at[0], b2_sem.at[1], q, e)
        own_in[0] = own_out[p]
        landed = own_in.at[1:n_dp]
        wait(landed, b2_sem.at[1])
        for k in range(n_dp):
            place(step_from(p, k, n_dp), own_in[k].astype(F32))
        wait(arrived, b1_sem.at[0])
        wait(landed, b2_sem.at[0])

    wait(slab_out.at[1:n_dp], s1_send)
    wait(slabs.at[1:pairs, 0], s2_send)
    wait(slabs.at[:, 0], s3_send)
    for n in range(n_b):
        wait(part_out[n], rs_send.at[n])
        wait(act_in[n], ag_send.at[n])
    wait(hid_in, hg_sem.at[0])


def store_kernel(wg_ref, ig_ref, wg_hbm, ig_hbm, sems):
    copies = [pltpu.make_async_copy(ig_ref, ig_hbm, sems.at[3])]
    for m in range(3):
        copies.append(pltpu.make_async_copy(wg_ref.at[m], wg_hbm.at[m], sems.at[m]))
    for copy in copies:
        copy.start()
    for copy in copies:
        copy.wait()


def per_device(n_dp, n_ex, out_grad, layer_input, expert_ids, gate_prob, w_stack, scale_exps):
    tok, width = out_grad.shape
    _, depth, hid = w_stack.shape
    batches = plan_batches(n_dp, n_ex, hid)
    total = sum(b.all for b in batches)
    n_b = len(batches)
    most = max(b.n_chunk for b in batches)
    pairs = n_ex // 2
    packed = (2, CAP * depth // 2)
    direct = n_dp * n_ex <= DIRECT
    vm = pl.BlockSpec(memory_space=pltpu.VMEM)
    dma = pltpu.SemaphoreType.DMA
    weight_grads, input_grad = pl.pallas_call(
        functools.partial(exchange_kernel, n_dp, n_ex, batches),
        out_shape=(
            jax.ShapeDtypeStruct((3, depth, hid), F32),
            jax.ShapeDtypeStruct((tok, width), BF),
        ),
        in_specs=[pl.BlockSpec(memory_space=pltpu.HBM)] * 6,
        out_specs=(vm, vm),
        scratch_shapes=[
            pltpu.VMEM((tok, width), BF),
            pltpu.VMEM((tok, width), BF),
            pltpu.VMEM((2, tok), jnp.int32),
            pltpu.VMEM((2, tok), F32),
            pltpu.SMEM(scale_exps.shape, jnp.int32),
            pltpu.VMEM((2, depth, total), BF),
            pltpu.VMEM((3, total, hid), BF),
            pltpu.VMEM((3, depth, hid), BF),
            pltpu.VMEM((n_dp, 8, depth), BF),
            pltpu.VMEM((pairs, 2, n_dp, 8, depth), BF),
            pltpu.VMEM((2, total, depth), BF),
            pltpu.VMEM((batches[-1].padded, hid), BF),
            pltpu.VMEM((n_dp, batches[-1].padded, hid), BF),
            pltpu.VMEM((total, depth), F32),
            pltpu.VMEM((n_ex, n_dp) + packed, BF),
            pltpu.VMEM(((n_ex * n_dp,) if direct else (n_ex, n_dp)) + packed, BF),
            pltpu.VMEM((n_dp,) + packed, BF),
            pltpu.VMEM((n_dp,) + packed, BF),
            dma((6,)),
            dma, dma((n_dp,)),
            dma, dma((pairs,)),
            dma, dma((pairs,)),
            pltpu.SemaphoreType.REGULAR((pairs,)),
            dma((n_b,)), dma((n_b, most)),
            dma((n_b,)), dma((n_b, most)),
            dma((2,)), dma((2,)), dma((2,)),
        ]
        + [pltpu.VMEM((b.n_chunk, n_dp, b.sum_rows, b.chunk), BF) for b in batches]
        + [pltpu.VMEM((b.n_chunk, n_dp, b.sum_rows, b.chunk), BF) for b in batches]
        + [pltpu.VMEM((b.n_chunk, b.act_rows, b.chunk), BF) for b in batches]
        + [pltpu.VMEM((b.n_chunk, n_dp, b.act_rows, b.chunk), BF) for b in batches],
        compiler_params=pltpu.CompilerParams(
            collective_id=0, has_side_effects=True, vmem_limit_bytes=VMEM_LIMIT
        ),
    )(*(
        pltpu.with_memory_space_constraint(v, pltpu.HBM)
        for v in (out_grad, layer_input, expert_ids.T, gate_prob.T, scale_exps, w_stack)
    ))
    weight_grads, input_grad = pl.pallas_call(
        store_kernel,
        in_specs=[vm, vm],
        out_specs=(pl.BlockSpec(memory_space=pl.ANY), pl.BlockSpec(memory_space=pl.ANY)),
        out_shape=(
            jax.ShapeDtypeStruct((3, depth, hid), F32),
            jax.ShapeDtypeStruct((tok, width), BF),
        ),
        scratch_shapes=[dma((4,))],
        compiler_params=pltpu.CompilerParams(vmem_limit_bytes=VMEM_LIMIT),
    )(weight_grads, input_grad)
    return input_grad, weight_grads


def solution(mesh):
    in_specs = (
        P(("dp", "expert"), None),
        P(("dp", "expert"), None),
        P(("dp", "expert"), None),
        P(("dp", "expert"), None),
        P(None, "dp", "expert"),
        P(None, "dp", "expert"),
    )
    out_specs = (P(("dp", "expert"), None), P(None, "dp", "expert"))
    return jax.shard_map(
        functools.partial(per_device, mesh.shape["dp"], mesh.shape["expert"]),
        mesh=mesh, in_specs=in_specs, out_specs=out_specs, check_vma=False,
    )
```

```python
import functools

import jax
import jax.numpy as jnp
from jax import lax
from jax.experimental import pallas as pl
from jax.experimental.pallas import tpu as pltpu
from jax.sharding import PartitionSpec as P

TILE = 128
CAP = 3
DIRECT = 64
TALL = 256
BF = jnp.bfloat16
F32 = jnp.float32
VMEM_LIMIT = 40 * 1024 * 1024


def iota(shape, dim):
    return lax.broadcasted_iota(jnp.int32, shape, dim)


def mm(a, b, ca=1, cb=0):
    return lax.dot_general(a, b, (((ca,), (cb,)), ((), ())), preferred_element_type=F32)


def up8(n):
    return -(-n // 8) * 8


def step_to(i, k, n):
    return i ^ k if n & (n - 1) == 0 else lax.rem(i + k, n)


def step_from(i, k, n):
    return i ^ k if n & (n - 1) == 0 else lax.rem(i - k + n, n)


def pad_rows(val, n):
    if val.shape[0] == n:
        return val
    return jnp.concatenate([val, jnp.zeros((n - val.shape[0], val.shape[1]), val.dtype)], axis=0)


class Batch:
    def __init__(self, steps, first, last, n_dp, hid):
        self.steps = steps
        self.rows = len(steps) * 2 * CAP
        self.padded = up8(self.rows)
        tight = up8(3 * self.rows) < 3 * self.padded
        self.stride = self.rows if tight else self.padded
        self.first = first
        self.last = last
        self.all = n_dp * self.padded
        self.local = first // n_dp
        self.sum_rows = up8(3 * self.stride)
        self.act_rows = up8(2 * self.stride)
        self.chunk = min(128, hid) if last else hid
        self.n_chunk = hid // self.chunk

    def cols(self, c):
        return slice(c * self.chunk, (c + 1) * self.chunk)


def plan_batches(n_dp, n_ex, hid):
    pairs = n_ex // 2
    groups = [[0], list(range(1, pairs))] if 1 < pairs <= 4 else [list(range(pairs))]
    batches, first = [], 0
    for i, steps in enumerate(groups):
        batches.append(Batch(steps, first, i == len(groups) - 1, n_dp, hid))
        first += batches[-1].all
        batches[-1].slot = sum(b.n_chunk for b in batches[:-1])
    return batches


def exchange_kernel(
    n_dp, n_ex, batches,
    og_hbm, li_hbm, ids_hbm, prob_hbm, exps_hbm, w_hbm,
    wg_ref, ig_ref, *scratch,
):
    n_b = len(batches)
    (
        og_ref, li_ref, ids_ref, prob_ref, exps_ref, xt, act, w, slab_out, slabs, x, hid_out, hid_in,
        acc, back_out, back_in, own_out, own_in,
        in_sem, s1_send, s1_recv, s2_send, s2_recv, s3_send, s3_recv, ready,
        rs_send, rs_recv, ag_send, ag_recv, hg_sem, b1_sem, b2_sem,
    ) = scratch[:33]
    bufs = scratch[33:]
    part_out, part_in, act_out, act_in = (bufs[i * n_b:(i + 1) * n_b] for i in range(4))
    p, e = lax.axis_index("dp"), lax.axis_index("expert")
    tok, width = og_hbm.shape
    _, depth, hid = w.shape
    pairs = n_ex // 2
    z, core = e // 2, e % 2
    other = 1 - core
    partner = 2 * z + other

    def send(src, dst, ssem, rsem, q, f):
        pltpu.make_async_remote_copy(
            src_ref=src, dst_ref=dst, send_sem=ssem, recv_sem=rsem,
            device_id=(q, f), device_id_type=pl.DeviceIdType.MESH,
        ).start()

    def wait(ref, sem):
        pltpu.make_async_copy(ref, ref, sem).wait()

    def tell(sem, q, f):
        pl.semaphore_signal(sem, inc=1, device_id=(q, f), device_id_type=pl.DeviceIdType.MESH)

    in_copies = [
        pltpu.make_async_copy(src, dst, in_sem.at[i])
        for i, (src, dst) in enumerate((
            (ids_hbm, ids_ref), (prob_hbm, prob_ref), (li_hbm, li_ref),
            (og_hbm, og_ref), (exps_hbm, exps_ref),
            (w_hbm.at[0], w.at[0]), (w_hbm.at[1], w.at[1]), (w_hbm.at[2], w.at[2]),
        ))
    ]
    for copy in in_copies[:5]:
        copy.start()

    barrier = pltpu.get_barrier_semaphore()
    for k in range(1, n_dp):
        tell(barrier, step_from(p, k, n_dp), partner)
    tell(barrier, p, partner)
    for j in range(1, pairs):
        s = step_from(z, j, pairs)

        @pl.when(s > z)
        def _(s=s):
            tell(barrier, p, 2 * s + other)

    for copy in in_copies[:4]:
        copy.wait()
    for copy in in_copies[5:]:
        copy.start()
    routed = ids_ref[...] == 0
    mask = jnp.max(routed.astype(F32), axis=0, keepdims=True)
    prob = jnp.sum(jnp.where(routed, prob_ref[...], 0.0), axis=0, keepdims=True)
    earlier = (iota((tok, tok), 0) <= iota((tok, tok), 1)).astype(BF)
    place = mm(jnp.broadcast_to(mask, (8, tok)).astype(BF), earlier) - 1.0
    mask_tall = jnp.broadcast_to(mask, (8, tok)) > 0.5
    row = iota((8, tok), 0).astype(F32)
    hit_in = jnp.where((place == row) & (row < CAP) & mask_tall, 1.0, 0.0)
    hit_gr = jnp.where((place + CAP == row) & (row >= CAP) & mask_tall, 1.0, 0.0)
    row_prob = jnp.sum(hit_gr * prob, axis=1, keepdims=True)
    slots = (
        mm(hit_in.astype(BF), li_ref[...]) + row_prob * mm(hit_gr.astype(BF), og_ref[...])
    ).astype(BF)
    for q in range(n_dp):
        slab_out[q] = slots[:, q * depth:(q + 1) * depth]
    pl.semaphore_wait(barrier, n_dp + z)

    for k in range(n_dp - 1, 0, -1):
        q = step_to(p, k, n_dp)
        send(slab_out.at[q], slabs.at[z, other, p], s1_send, s1_recv.at[k], q, partner)
    for j in range(1, pairs):
        s = step_from(z, j, pairs)

        @pl.when(s < z)
        def _(s=s, j=j):
            tell(ready.at[j], p, 2 * s + other)

    slabs[z, core, p] = slab_out[p]

    def forward_down(src):
        for j in range(pairs - 1, 0, -1):
            t = step_to(z, j, pairs)

            @pl.when(t < z)
            def _(t=t, j=j):
                send(src, src, s2_send, s2_recv.at[j], p, 2 * t + other)

    fine = n_dp <= 4
    if fine:
        forward_down(slabs.at[z, core, p])

    in_copies[4].wait()
    tr, tc = depth // TILE, hid // TILE

    def scale_rows(m, r, carry):
        at = pl.ds(pl.multiple_of(r * TILE, TILE), TILE)
        for j in range(tc):
            power = lax.shift_left(jnp.int32(1), exps_ref[m, r, j] + 15)
            factor = power.astype(F32) * (2.0 ** -15)
            cols = slice(j * TILE, (j + 1) * TILE)
            w[m, at, cols] = (w[m, at, cols].astype(F32) * factor).astype(BF)
        return carry

    for m in range(3):
        in_copies[5 + m].wait()
        lax.fori_loop(0, tr, functools.partial(scale_rows, m), 0)

    for k in range(1, n_dp):
        q = step_from(p, k, n_dp)
        wait(slabs.at[z, core, q], s1_recv.at[k])
        if fine:
            forward_down(slabs.at[z, core, q])
    held = slabs.at[z, core]
    send(held, held, s3_send, s3_recv.at[0], p, partner)
    if not fine:
        forward_down(held)
    for j in range(1, pairs):
        t = step_to(z, j, pairs)

        @pl.when(t > z)
        def _(t=t, j=j):
            pl.semaphore_wait(ready.at[j], 1)
            send(held, held, s2_send, s2_recv.at[j], p, 2 * t + other)

    def pass_on(b):
        for j in b.steps:
            if j:
                block = slabs.at[step_from(z, j, pairs), other]
                wait(block, s2_recv.at[j])
                send(block, block, s3_send, s3_recv.at[j], p, partner)

    def collect(b):
        for j in b.steps:
            s = step_from(z, j, pairs)
            wait(slabs.at[s, core if j else other], s3_recv.at[j])
        shape = (2 * b.padded, len(b.steps) * 16)
        src, dst = iota(shape, 1), iota(shape, 0)
        kind, r = dst // b.padded, dst % b.padded
        jl, cs, c = r // (2 * CAP), (r // CAP) % 2, r % CAP
        rows = [[], []]
        for g in range(n_dp):
            h = jnp.where(g == p, cs, 1 - cs)
            pick = jnp.where(
                (src == jl * 16 + h * 8 + kind * CAP + c) & (r < b.rows), 1.0, 0.0
            ).astype(BF)
            have = jnp.concatenate(
                [slabs[step_from(z, j, pairs), :, g].reshape(16, depth) for j in b.steps], axis=0
            )
            val = mm(pick, have)
            for i in range(2):
                rows[i].append(val[i * b.padded:(i + 1) * b.padded])
        for i in range(2):
            x[i, b.first:b.first + b.all] = jnp.concatenate(rows[i], axis=0).astype(BF)

    def multiply(n, c):
        b = batches[n]
        vals = [
            mm(x[m // 2, b.first:b.first + b.all], w[m, :, b.cols(c)]) for m in range(3)
        ]
        for g in range(n_dp):
            at = g * b.padded
            block = jnp.concatenate([v[at:at + b.stride] for v in vals], axis=0)
            part_out[n][c, g] = pad_rows(block, b.sum_rows).astype(BF)
        for k in range(n_dp - 1, -1, -1):
            q = step_to(p, k, n_dp)
            send(part_out[n].at[c, q], part_in[n].at[c, p], rs_send.at[n], rs_recv.at[b.slot + c], q, partner)

    def activate(n, c):
        b = batches[n]
        wait(part_in[n].at[c], rs_recv.at[b.slot + c])
        total = part_in[n][c, 0].astype(F32)
        for g in range(1, n_dp):
            total = total + part_in[n][c, g].astype(F32)
        gate, up, down = (total[m * b.stride:(m + 1) * b.stride] for m in range(3))
        sig = jax.nn.sigmoid(gate)
        silu = gate * sig
        grads = [down * up * sig * (1.0 + gate * (1.0 - sig)), down * silu]
        hid_out[b.local:b.local + b.padded, b.cols(c)] = pad_rows(silu * up, b.padded).astype(BF)
        act_out[n][c] = pad_rows(jnp.concatenate(grads, axis=0), b.act_rows).astype(BF)
        for k in range(n_dp - 1, -1, -1):
            q = step_to(p, k, n_dp)
            send(
                act_out[n].at[c], act_in[n].at[c, p], ag_send.at[n], ag_recv.at[b.slot + c],
                q, partner,
            )

    if n_b == 1:
        pass_on(batches[0])
    collect(batches[0])
    if n_b > 1:
        multiply(0, 0)
        pass_on(batches[1])
        activate(0, 0)
        collect(batches[1])
    for c in range(batches[-1].n_chunk):
        multiply(n_b - 1, c)

    for i in range(2):
        xt[i] = x[i].astype(F32).T.astype(BF)

    for n, b in list(enumerate(batches))[-1:]:
        for c in range(b.n_chunk):
            activate(n, c)
    for k in range(n_dp - 1, -1, -1):
        send(hid_out, hid_in.at[p], hg_sem.at[0], hg_sem.at[1], step_to(p, k, n_dp), partner)

    def unpack(n, c):
        b = batches[n]
        wait(act_in[n].at[c], ag_recv.at[b.slot + c])
        blocks = [act_in[n][c, g].astype(F32) for g in range(n_dp)]
        for m in range(2):
            val = [pad_rows(v[m * b.stride:(m + 1) * b.stride], b.padded) for v in blocks]
            act[m, b.first:b.first + b.all, b.cols(c)] = jnp.concatenate(val, axis=0).astype(BF)

    for n, b in enumerate(batches):
        for c in range(b.n_chunk):
            unpack(n, c)
            if b.last:
                cols = b.cols(c)
                part = mm(act[0, :, cols], w[0, :, cols], 1, 1) + mm(act[1, :, cols], w[1, :, cols], 1, 1)
                if c == 0:
                    acc[...] = part
                else:
                    acc[...] += part

    pad = n_dp * 2
    half = depth // 2
    summed = acc[...].astype(BF)
    some = min(n_ex, 8)
    for i in range(n_ex // some):
        shape = (some * pad, summed.shape[0])
        to, frm = iota(shape, 0), iota(shape, 1)
        f, g = to // pad + i * some, (to % pad) // 2
        cs = jnp.where(core == 0, f % 2, 1 - f % 2)
        if n_b == 1:
            base = g * batches[0].padded + (f // 2) * 2 * CAP
        else:
            base = 0
            for b in batches:
                for jl, j in enumerate(b.steps):
                    base = jnp.where(f // 2 == j, b.first + g * b.padded + jl * 2 * CAP, base)
        base = base + cs * CAP
        parts = []
        for t in range(CAP):
            piece = CAP * (to % 2) + t
            val = 0.0
            for h in range(2):
                choose = jnp.where(
                    (piece % 2 == h) & (frm == base + piece // 2), 1.0, 0.0
                ).astype(BF)
                val = val + mm(choose, summed[:, h * half:(h + 1) * half])
            parts.append(val)
        val = jnp.concatenate(parts, axis=1)
        for j in range(some):
            for g in range(n_dp):
                at = j * pad + g * 2
                back_out[i * some + j, g] = val[at:at + 2].astype(BF)

    tall = min(TALL, depth)

    def weight_grads():
        for m in range(3):
            if m == 2:
                wait(hid_in, hg_sem.at[1])
                for b in batches:
                    act[2, b.first:b.first + b.all] = jnp.concatenate(
                        [hid_in[g, b.local:b.local + b.padded].astype(F32) for g in range(n_dp)],
                        axis=0,
                    ).astype(BF)
            for r in range(0, depth, tall):
                at = slice(r, r + tall)
                wg_ref[m, at, :] = mm(xt[m // 2, at, :], act[m])

    def place(q, packed):
        halves = [
            packed[j // CAP:j // CAP + 1, (j % CAP) * half:(j % CAP + 1) * half]
            for j in range(2 * CAP)
        ]
        back_rows = jnp.concatenate(
            [jnp.concatenate(halves[2 * c:2 * c + 2], axis=1) for c in range(CAP)], axis=0
        ).astype(BF)
        ig_ref[:, pl.ds(pl.multiple_of(q * depth, TILE), depth)] = mm(
            hit_in[:CAP].astype(BF), back_rows, 0, 0
        ).astype(BF)

    def far(k):
        return 2 * step_to(z, k // 2, pairs) + (core ^ (k % 2))

    if n_dp * n_ex <= DIRECT:
        for r in range(n_ex * n_dp - 1, 0, -1):
            q = step_to(p, r % n_dp, n_dp)
            send(
                back_out.at[r // n_dp, q], back_in.at[r], b1_sem.at[0], b1_sem.at[1],
                q, far(r // n_dp),
            )
        back_in[0] = back_out[0, p]
        weight_grads()
        arrived = back_in.at[1:n_ex * n_dp]
        wait(arrived, b1_sem.at[1])
        for k in range(n_dp):
            total = back_in[k].astype(F32)
            for f in range(1, n_ex):
                total = total + back_in[f * n_dp + k].astype(F32)
            place(step_from(p, k, n_dp), total)
        wait(arrived, b1_sem.at[0])
    else:
        for k in range(1, n_ex):
            send(back_out.at[k], back_in.at[k], b1_sem.at[0], b1_sem.at[1], p, far(k))
        weight_grads()
        arrived = back_in.at[1:n_ex]
        wait(arrived, b1_sem.at[1])
        for g in range(n_dp):
            total = back_out[0, g].astype(F32)
            for k in range(1, n_ex):
                total = total + back_in[k, g].astype(F32)
            own_out[g] = total.astype(BF)
        for k in range(1, n_dp):
            q = step_to(p, k, n_dp)
            send(own_out.at[q], own_in.at[k], b2_sem.at[0], b2_sem.at[1], q, e)
        own_in[0] = own_out[p]
        landed = own_in.at[1:n_dp]
        wait(landed, b2_sem.at[1])
        for k in range(n_dp):
            place(step_from(p, k, n_dp), own_in[k].astype(F32))
        wait(arrived, b1_sem.at[0])
        wait(landed, b2_sem.at[0])

    wait(slab_out.at[1:n_dp], s1_send)
    wait(slabs.at[1:pairs, 0], s2_send)
    wait(slabs.at[:, 0], s3_send)
    for n in range(n_b):
        wait(part_out[n], rs_send.at[n])
        wait(act_in[n], ag_send.at[n])
    wait(hid_in, hg_sem.at[0])


def store_kernel(wg_ref, ig_ref, wg_hbm, ig_hbm, sems):
    copies = [pltpu.make_async_copy(ig_ref, ig_hbm, sems.at[3])]
    for m in range(3):
        copies.append(pltpu.make_async_copy(wg_ref.at[m], wg_hbm.at[m], sems.at[m]))
    for copy in copies:
        copy.start()
    for copy in copies:
        copy.wait()


def per_device(n_dp, n_ex, out_grad, layer_input, expert_ids, gate_prob, w_stack, scale_exps):
    tok, width = out_grad.shape
    _, depth, hid = w_stack.shape
    batches = plan_batches(n_dp, n_ex, hid)
    total = sum(b.all for b in batches)
    n_b = len(batches)
    parts = sum(b.n_chunk for b in batches)
    pairs = n_ex // 2
    packed = (2, CAP * depth // 2)
    direct = n_dp * n_ex <= DIRECT
    vm = pl.BlockSpec(memory_space=pltpu.VMEM)
    dma = pltpu.SemaphoreType.DMA
    weight_grads, input_grad = pl.pallas_call(
        functools.partial(exchange_kernel, n_dp, n_ex, batches),
        out_shape=(
            jax.ShapeDtypeStruct((3, depth, hid), F32),
            jax.ShapeDtypeStruct((tok, width), BF),
        ),
        in_specs=[pl.BlockSpec(memory_space=pltpu.HBM)] * 6,
        out_specs=(vm, vm),
        scratch_shapes=[
            pltpu.VMEM((tok, width), BF),
            pltpu.VMEM((tok, width), BF),
            pltpu.VMEM((2, tok), jnp.int32),
            pltpu.VMEM((2, tok), F32),
            pltpu.SMEM(scale_exps.shape, jnp.int32),
            pltpu.VMEM((2, depth, total), BF),
            pltpu.VMEM((3, total, hid), BF),
            pltpu.VMEM((3, depth, hid), BF),
            pltpu.VMEM((n_dp, 8, depth), BF),
            pltpu.VMEM((pairs, 2, n_dp, 8, depth), BF),
            pltpu.VMEM((2, total, depth), BF),
            pltpu.VMEM((total // n_dp, hid), BF),
            pltpu.VMEM((n_dp, total // n_dp, hid), BF),
            pltpu.VMEM((total, depth), F32),
            pltpu.VMEM((n_ex, n_dp) + packed, BF),
            pltpu.VMEM(((n_ex * n_dp,) if direct else (n_ex, n_dp)) + packed, BF),
            pltpu.VMEM((n_dp,) + packed, BF),
            pltpu.VMEM((n_dp,) + packed, BF),
            dma((8,)),
            dma, dma((n_dp,)),
            dma, dma((pairs,)),
            dma, dma((pairs,)),
            pltpu.SemaphoreType.REGULAR((pairs,)),
            dma((n_b,)), dma((parts,)),
            dma((n_b,)), dma((parts,)),
            dma((2,)), dma((2,)), dma((2,)),
        ]
        + [pltpu.VMEM((b.n_chunk, n_dp, b.sum_rows, b.chunk), BF) for b in batches]
        + [pltpu.VMEM((b.n_chunk, n_dp, b.sum_rows, b.chunk), BF) for b in batches]
        + [pltpu.VMEM((b.n_chunk, b.act_rows, b.chunk), BF) for b in batches]
        + [pltpu.VMEM((b.n_chunk, n_dp, b.act_rows, b.chunk), BF) for b in batches],
        compiler_params=pltpu.CompilerParams(
            collective_id=0, has_side_effects=True, vmem_limit_bytes=VMEM_LIMIT
        ),
    )(*(
        pltpu.with_memory_space_constraint(v, pltpu.HBM)
        for v in (out_grad, layer_input, expert_ids.T, gate_prob.T, scale_exps, w_stack)
    ))
    weight_grads, input_grad = pl.pallas_call(
        store_kernel,
        in_specs=[vm, vm],
        out_specs=(pl.BlockSpec(memory_space=pl.ANY), pl.BlockSpec(memory_space=pl.ANY)),
        out_shape=(
            jax.ShapeDtypeStruct((3, depth, hid), F32),
            jax.ShapeDtypeStruct((tok, width), BF),
        ),
        scratch_shapes=[dma((4,))],
        compiler_params=pltpu.CompilerParams(vmem_limit_bytes=VMEM_LIMIT),
    )(weight_grads, input_grad)
    return input_grad, weight_grads


def solution(mesh):
    in_specs = (
        P(("dp", "expert"), None),
        P(("dp", "expert"), None),
        P(("dp", "expert"), None),
        P(("dp", "expert"), None),
        P(None, "dp", "expert"),
        P(None, "dp", "expert"),
    )
    out_specs = (P(("dp", "expert"), None), P(None, "dp", "expert"))
    return jax.shard_map(
        functools.partial(per_device, mesh.shape["dp"], mesh.shape["expert"]),
        mesh=mesh, in_specs=in_specs, out_specs=out_specs, check_vma=False,
    )
```

```python
import functools

import jax
import jax.numpy as jnp
from jax import lax
from jax.experimental import pallas as pl
from jax.experimental.pallas import tpu as pltpu
from jax.sharding import PartitionSpec as P

TILE = 128
CAP = 3
DIRECT = 64
TALL = 256
BF = jnp.bfloat16
F32 = jnp.float32
VMEM_LIMIT = 40 * 1024 * 1024


def iota(shape, dim):
    return lax.broadcasted_iota(jnp.int32, shape, dim)


def mm(a, b, ca=1, cb=0):
    return lax.dot_general(a, b, (((ca,), (cb,)), ((), ())), preferred_element_type=F32)


def up8(n):
    return -(-n // 8) * 8


def step_to(i, k, n):
    return i ^ k if n & (n - 1) == 0 else lax.rem(i + k, n)


def steps_between(i, t, n):
    return i ^ t if n & (n - 1) == 0 else lax.rem(t - i + n, n)


def step_from(i, k, n):
    return i ^ k if n & (n - 1) == 0 else lax.rem(i - k + n, n)


def pad_rows(val, n):
    if val.shape[0] == n:
        return val
    return jnp.concatenate([val, jnp.zeros((n - val.shape[0], val.shape[1]), val.dtype)], axis=0)


class Batch:
    def __init__(self, steps, first, last, n_dp, hid):
        self.steps = steps
        self.rows = len(steps) * 2 * CAP
        self.padded = up8(self.rows)
        tight = up8(3 * self.rows) < 3 * self.padded
        self.stride = self.rows if tight else self.padded
        self.first = first
        self.last = last
        self.all = n_dp * self.padded
        self.local = first // n_dp
        self.sum_rows = up8(3 * self.stride)
        self.act_rows = up8(2 * self.stride)
        self.chunk = min(128, hid) if last else hid
        self.n_chunk = hid // self.chunk

    def cols(self, c):
        return slice(c * self.chunk, (c + 1) * self.chunk)


def plan_batches(n_dp, n_ex, hid):
    pairs = n_ex // 2
    groups = [[0], list(range(1, pairs))] if 1 < pairs <= 4 else [list(range(pairs))]
    batches, first = [], 0
    for i, steps in enumerate(groups):
        batches.append(Batch(steps, first, i == len(groups) - 1, n_dp, hid))
        first += batches[-1].all
        batches[-1].slot = sum(b.n_chunk for b in batches[:-1])
    return batches


def exchange_kernel(
    n_dp, n_ex, batches,
    og_hbm, li_hbm, ids_hbm, prob_hbm, exps_hbm, w_hbm,
    wg_ref, ig_ref, *scratch,
):
    n_b = len(batches)
    (
        og_ref, li_ref, ids_ref, prob_ref, exps_ref, xt, act, w, slab_out, slabs, x, hid_out, hid_in,
        acc, back_out, back_in, own_out, own_in,
        in_sem, s1_send, s1_recv, s2_send, s2_recv, s3_send, s3_recv, ready,
        rs_send, rs_recv, ag_send, ag_recv, hg_sem, b1_sem, b2_sem,
    ) = scratch[:33]
    bufs = scratch[33:]
    part_out, part_in, act_out, act_in = (bufs[i * n_b:(i + 1) * n_b] for i in range(4))
    p, e = lax.axis_index("dp"), lax.axis_index("expert")
    tok, width = og_hbm.shape
    _, depth, hid = w.shape
    pairs = n_ex // 2
    z, core = e // 2, e % 2
    other = 1 - core
    partner = 2 * z + other

    def send(src, dst, ssem, rsem, q, f):
        pltpu.make_async_remote_copy(
            src_ref=src, dst_ref=dst, send_sem=ssem, recv_sem=rsem,
            device_id=(q, f), device_id_type=pl.DeviceIdType.MESH,
        ).start()

    def wait(ref, sem):
        pltpu.make_async_copy(ref, ref, sem).wait()

    def tell(sem, q, f):
        pl.semaphore_signal(sem, inc=1, device_id=(q, f), device_id_type=pl.DeviceIdType.MESH)

    in_copies = [
        pltpu.make_async_copy(src, dst, in_sem.at[i])
        for i, (src, dst) in enumerate((
            (ids_hbm, ids_ref), (prob_hbm, prob_ref), (li_hbm, li_ref),
            (og_hbm, og_ref), (exps_hbm, exps_ref),
            (w_hbm.at[0], w.at[0]), (w_hbm.at[1], w.at[1]), (w_hbm.at[2], w.at[2]),
        ))
    ]
    for copy in in_copies[:5]:
        copy.start()

    barrier = pltpu.get_barrier_semaphore()
    for k in range(1, n_dp):
        tell(barrier, step_from(p, k, n_dp), partner)
    tell(barrier, p, partner)
    for j in range(1, pairs):
        s = step_from(z, j, pairs)

        @pl.when(s > z)
        def _(s=s):
            tell(barrier, p, 2 * s + other)

    for copy in in_copies[:4]:
        copy.wait()
    for copy in in_copies[5:]:
        copy.start()
    routed = ids_ref[...] == 0
    mask = jnp.max(routed.astype(F32), axis=0, keepdims=True)
    prob = jnp.sum(jnp.where(routed, prob_ref[...], 0.0), axis=0, keepdims=True)
    earlier = (iota((tok, tok), 0) <= iota((tok, tok), 1)).astype(BF)
    place = mm(jnp.broadcast_to(mask, (8, tok)).astype(BF), earlier) - 1.0
    mask_tall = jnp.broadcast_to(mask, (8, tok)) > 0.5
    row = iota((8, tok), 0).astype(F32)
    hit_in = jnp.where((place == row) & (row < CAP) & mask_tall, 1.0, 0.0)
    hit_gr = jnp.where((place + CAP == row) & (row >= CAP) & mask_tall, 1.0, 0.0)
    row_prob = jnp.sum(hit_gr * prob, axis=1, keepdims=True)
    slots = (
        mm(hit_in.astype(BF), li_ref[...]) + row_prob * mm(hit_gr.astype(BF), og_ref[...])
    ).astype(BF)
    for q in range(n_dp):
        slab_out[q] = slots[:, q * depth:(q + 1) * depth]
    pl.semaphore_wait(barrier, n_dp + z)

    for k in range(n_dp - 1, 0, -1):
        q = step_to(p, k, n_dp)
        send(slab_out.at[q], slabs.at[z, other, p], s1_send, s1_recv.at[k], q, partner)
    for j in range(1, pairs):
        s = step_from(z, j, pairs)

        @pl.when(s < z)
        def _(s=s, j=j):
            tell(ready.at[j], p, 2 * s + other)

    slabs[z, core, p] = slab_out[p]

    def forward_down(src):
        for j in range(pairs - 1, 0, -1):
            t = step_to(z, j, pairs)

            @pl.when(t < z)
            def _(t=t, j=j):
                send(src, src, s2_send, s2_recv.at[j], p, 2 * t + other)

    fine = n_dp <= 4
    if fine:
        forward_down(slabs.at[z, core, p])

    in_copies[4].wait()
    tr, tc = depth // TILE, hid // TILE

    def scale_rows(m, r, carry):
        at = pl.ds(pl.multiple_of(r * TILE, TILE), TILE)
        for j in range(tc):
            power = lax.shift_left(jnp.int32(1), exps_ref[m, r, j] + 15)
            factor = power.astype(F32) * (2.0 ** -15)
            cols = slice(j * TILE, (j + 1) * TILE)
            w[m, at, cols] = (w[m, at, cols].astype(F32) * factor).astype(BF)
        return carry

    for m in range(3):
        in_copies[5 + m].wait()
        lax.fori_loop(0, tr, functools.partial(scale_rows, m), 0)

    for k in range(1, n_dp):
        q = step_from(p, k, n_dp)
        wait(slabs.at[z, core, q], s1_recv.at[k])
        if fine:
            forward_down(slabs.at[z, core, q])
    held = slabs.at[z, core]
    send(held, held, s3_send, s3_recv.at[0], p, partner)
    if not fine:
        forward_down(held)
    for j in range(1, pairs):
        t = step_to(z, j, pairs)

        @pl.when(t > z)
        def _(t=t, j=j):
            pl.semaphore_wait(ready.at[j], 1)
            send(held, held, s2_send, s2_recv.at[j], p, 2 * t + other)

    def pass_on(b):
        for j in b.steps:
            if j:
                block = slabs.at[step_from(z, j, pairs), other]
                wait(block, s2_recv.at[j])
                send(block, block, s3_send, s3_recv.at[j], p, partner)

    def collect(b):
        for j in b.steps:
            s = step_from(z, j, pairs)
            wait(slabs.at[s, core if j else other], s3_recv.at[j])
        shape = (2 * b.padded, len(b.steps) * 16)
        src, dst = iota(shape, 1), iota(shape, 0)
        kind, r = dst // b.padded, dst % b.padded
        jl, cs, c = r // (2 * CAP), (r // CAP) % 2, r % CAP
        rows = [[], []]
        for g in range(n_dp):
            h = jnp.where(g == p, cs, 1 - cs)
            pick = jnp.where(
                (src == jl * 16 + h * 8 + kind * CAP + c) & (r < b.rows), 1.0, 0.0
            ).astype(BF)
            have = jnp.concatenate(
                [slabs[step_from(z, j, pairs), :, g].reshape(16, depth) for j in b.steps], axis=0
            )
            val = mm(pick, have)
            for i in range(2):
                rows[i].append(val[i * b.padded:(i + 1) * b.padded])
        for i in range(2):
            x[i, b.first:b.first + b.all] = jnp.concatenate(rows[i], axis=0).astype(BF)

    def multiply(n, c):
        b = batches[n]
        vals = [
            mm(x[m // 2, b.first:b.first + b.all], w[m, :, b.cols(c)]) for m in range(3)
        ]
        for g in range(n_dp):
            at = g * b.padded
            block = jnp.concatenate([v[at:at + b.stride] for v in vals], axis=0)
            part_out[n][c, g] = pad_rows(block, b.sum_rows).astype(BF)
        for k in range(n_dp - 1, -1, -1):
            q = step_to(p, k, n_dp)
            send(part_out[n].at[c, q], part_in[n].at[c, p], rs_send.at[n], rs_recv.at[b.slot + c], q, partner)

    def activate(n, c):
        b = batches[n]
        wait(part_in[n].at[c], rs_recv.at[b.slot + c])
        total = part_in[n][c, 0].astype(F32)
        for g in range(1, n_dp):
            total = total + part_in[n][c, g].astype(F32)
        gate, up, down = (total[m * b.stride:(m + 1) * b.stride] for m in range(3))
        sig = jax.nn.sigmoid(gate)
        silu = gate * sig
        grads = [down * up * sig * (1.0 + gate * (1.0 - sig)), down * silu]
        hid_out[b.local:b.local + b.padded, b.cols(c)] = pad_rows(silu * up, b.padded).astype(BF)
        act_out[n][c] = pad_rows(jnp.concatenate(grads, axis=0), b.act_rows).astype(BF)
        for k in range(n_dp - 1, -1, -1):
            q = step_to(p, k, n_dp)
            send(
                act_out[n].at[c], act_in[n].at[c, p], ag_send.at[n], ag_recv.at[b.slot + c],
                q, partner,
            )

    if n_b == 1:
        pass_on(batches[0])
    collect(batches[0])
    if n_b > 1:
        multiply(0, 0)
        pass_on(batches[1])
        activate(0, 0)
        collect(batches[1])
    for c in range(batches[-1].n_chunk):
        multiply(n_b - 1, c)

    for i in range(2):
        xt[i] = x[i].astype(F32).T.astype(BF)

    for n, b in list(enumerate(batches))[-1:]:
        for c in range(b.n_chunk):
            activate(n, c)
    for k in range(n_dp - 1, -1, -1):
        send(hid_out, hid_in.at[p], hg_sem.at[0], hg_sem.at[1], step_to(p, k, n_dp), partner)

    def unpack(n, c):
        b = batches[n]
        wait(act_in[n].at[c], ag_recv.at[b.slot + c])
        blocks = [act_in[n][c, g].astype(F32) for g in range(n_dp)]
        for m in range(2):
            val = [pad_rows(v[m * b.stride:(m + 1) * b.stride], b.padded) for v in blocks]
            act[m, b.first:b.first + b.all, b.cols(c)] = jnp.concatenate(val, axis=0).astype(BF)

    for n, b in enumerate(batches):
        for c in range(b.n_chunk):
            unpack(n, c)
            if b.last:
                cols = b.cols(c)
                part = mm(act[0, :, cols], w[0, :, cols], 1, 1) + mm(act[1, :, cols], w[1, :, cols], 1, 1)
                if c == 0:
                    acc[...] = part
                else:
                    acc[...] += part

    pad = n_dp * 2
    half = depth // 2
    summed = acc[...].astype(BF)
    some = min(n_ex, 8)
    for i in range(n_ex // some):
        shape = (some * pad, summed.shape[0])
        to, frm = iota(shape, 0), iota(shape, 1)
        f, g = to // pad + i * some, (to % pad) // 2
        cs = jnp.where(core == 0, f % 2, 1 - f % 2)
        if n_b == 1:
            base = g * batches[0].padded + (f // 2) * 2 * CAP
        else:
            base = 0
            for b in batches:
                for jl, j in enumerate(b.steps):
                    base = jnp.where(f // 2 == j, b.first + g * b.padded + jl * 2 * CAP, base)
        base = base + cs * CAP
        parts = []
        for t in range(CAP):
            piece = CAP * (to % 2) + t
            val = 0.0
            for h in range(2):
                choose = jnp.where(
                    (piece % 2 == h) & (frm == base + piece // 2), 1.0, 0.0
                ).astype(BF)
                val = val + mm(choose, summed[:, h * half:(h + 1) * half])
            parts.append(val)
        val = jnp.concatenate(parts, axis=1)
        for j in range(some):
            for g in range(n_dp):
                at = j * pad + g * 2
                back_out[i * some + j, g] = val[at:at + 2].astype(BF)

    tall = min(TALL, depth)

    def weight_grads():
        for m in range(3):
            if m == 2:
                wait(hid_in, hg_sem.at[1])
                for b in batches:
                    act[2, b.first:b.first + b.all] = jnp.concatenate(
                        [hid_in[g, b.local:b.local + b.padded].astype(F32) for g in range(n_dp)],
                        axis=0,
                    ).astype(BF)
            for r in range(0, depth, tall):
                at = slice(r, r + tall)
                wg_ref[m, at, :] = mm(xt[m // 2, at, :], act[m])

    def place(q, packed):
        halves = [
            packed[j // CAP:j // CAP + 1, (j % CAP) * half:(j % CAP + 1) * half]
            for j in range(2 * CAP)
        ]
        back_rows = jnp.concatenate(
            [jnp.concatenate(halves[2 * c:2 * c + 2], axis=1) for c in range(CAP)], axis=0
        ).astype(BF)
        ig_ref[:, pl.ds(pl.multiple_of(q * depth, TILE), depth)] = mm(
            hit_in[:CAP].astype(BF), back_rows, 0, 0
        ).astype(BF)

    def far(k):
        return 2 * step_to(z, k // 2, pairs) + (core ^ (k % 2))

    if n_dp * n_ex <= DIRECT:
        def give(q, f):
            k = 2 * steps_between(z, f // 2, pairs) + (core ^ (f % 2))
            send(
                back_out.at[k, q], back_in.at[k * n_dp + steps_between(p, q, n_dp)],
                b1_sem.at[0], b1_sem.at[1], q, f,
            )

        for f in range(2):
            @pl.when((p > 0) | (e != f))
            def _(f=f):
                give(0, f)

        for r in range(n_ex * n_dp - 1, 0, -1):
            q, f = step_to(p, r % n_dp, n_dp), far(r // n_dp)

            @pl.when((q > 0) | (f > 1))
            def _(q=q, f=f):
                give(q, f)

        back_in[0] = back_out[0, p]
        weight_grads()
        arrived = back_in.at[1:n_ex * n_dp]
        wait(arrived, b1_sem.at[1])
        for k in range(n_dp):
            total = back_in[k].astype(F32)
            for f in range(1, n_ex):
                total = total + back_in[f * n_dp + k].astype(F32)
            place(step_from(p, k, n_dp), total)
        wait(arrived, b1_sem.at[0])
    else:
        for k in range(1, n_ex):
            send(back_out.at[k], back_in.at[k], b1_sem.at[0], b1_sem.at[1], p, far(k))
        weight_grads()
        arrived = back_in.at[1:n_ex]
        wait(arrived, b1_sem.at[1])
        for g in range(n_dp):
            total = back_out[0, g].astype(F32)
            for k in range(1, n_ex):
                total = total + back_in[k, g].astype(F32)
            own_out[g] = total.astype(BF)
        for k in range(1, n_dp):
            q = step_to(p, k, n_dp)
            send(own_out.at[q], own_in.at[k], b2_sem.at[0], b2_sem.at[1], q, e)
        own_in[0] = own_out[p]
        landed = own_in.at[1:n_dp]
        wait(landed, b2_sem.at[1])
        for k in range(n_dp):
            place(step_from(p, k, n_dp), own_in[k].astype(F32))
        wait(arrived, b1_sem.at[0])
        wait(landed, b2_sem.at[0])

    wait(slab_out.at[1:n_dp], s1_send)
    wait(slabs.at[1:pairs, 0], s2_send)
    wait(slabs.at[:, 0], s3_send)
    for n in range(n_b):
        wait(part_out[n], rs_send.at[n])
        wait(act_in[n], ag_send.at[n])
    wait(hid_in, hg_sem.at[0])


def store_kernel(wg_ref, ig_ref, wg_hbm, ig_hbm, sems):
    copies = [pltpu.make_async_copy(ig_ref, ig_hbm, sems.at[3])]
    for m in range(3):
        copies.append(pltpu.make_async_copy(wg_ref.at[m], wg_hbm.at[m], sems.at[m]))
    for copy in copies:
        copy.start()
    for copy in copies:
        copy.wait()


def per_device(n_dp, n_ex, out_grad, layer_input, expert_ids, gate_prob, w_stack, scale_exps):
    tok, width = out_grad.shape
    _, depth, hid = w_stack.shape
    batches = plan_batches(n_dp, n_ex, hid)
    total = sum(b.all for b in batches)
    n_b = len(batches)
    parts = sum(b.n_chunk for b in batches)
    pairs = n_ex // 2
    packed = (2, CAP * depth // 2)
    direct = n_dp * n_ex <= DIRECT
    vm = pl.BlockSpec(memory_space=pltpu.VMEM)
    dma = pltpu.SemaphoreType.DMA
    weight_grads, input_grad = pl.pallas_call(
        functools.partial(exchange_kernel, n_dp, n_ex, batches),
        out_shape=(
            jax.ShapeDtypeStruct((3, depth, hid), F32),
            jax.ShapeDtypeStruct((tok, width), BF),
        ),
        in_specs=[pl.BlockSpec(memory_space=pltpu.HBM)] * 6,
        out_specs=(vm, vm),
        scratch_shapes=[
            pltpu.VMEM((tok, width), BF),
            pltpu.VMEM((tok, width), BF),
            pltpu.VMEM((2, tok), jnp.int32),
            pltpu.VMEM((2, tok), F32),
            pltpu.SMEM(scale_exps.shape, jnp.int32),
            pltpu.VMEM((2, depth, total), BF),
            pltpu.VMEM((3, total, hid), BF),
            pltpu.VMEM((3, depth, hid), BF),
            pltpu.VMEM((n_dp, 8, depth), BF),
            pltpu.VMEM((pairs, 2, n_dp, 8, depth), BF),
            pltpu.VMEM((2, total, depth), BF),
            pltpu.VMEM((total // n_dp, hid), BF),
            pltpu.VMEM((n_dp, total // n_dp, hid), BF),
            pltpu.VMEM((total, depth), F32),
            pltpu.VMEM((n_ex, n_dp) + packed, BF),
            pltpu.VMEM(((n_ex * n_dp,) if direct else (n_ex, n_dp)) + packed, BF),
            pltpu.VMEM((n_dp,) + packed, BF),
            pltpu.VMEM((n_dp,) + packed, BF),
            dma((8,)),
            dma, dma((n_dp,)),
            dma, dma((pairs,)),
            dma, dma((pairs,)),
            pltpu.SemaphoreType.REGULAR((pairs,)),
            dma((n_b,)), dma((parts,)),
            dma((n_b,)), dma((parts,)),
            dma((2,)), dma((2,)), dma((2,)),
        ]
        + [pltpu.VMEM((b.n_chunk, n_dp, b.sum_rows, b.chunk), BF) for b in batches]
        + [pltpu.VMEM((b.n_chunk, n_dp, b.sum_rows, b.chunk), BF) for b in batches]
        + [pltpu.VMEM((b.n_chunk, b.act_rows, b.chunk), BF) for b in batches]
        + [pltpu.VMEM((b.n_chunk, n_dp, b.act_rows, b.chunk), BF) for b in batches],
        compiler_params=pltpu.CompilerParams(
            collective_id=0, has_side_effects=True, vmem_limit_bytes=VMEM_LIMIT
        ),
    )(*(
        pltpu.with_memory_space_constraint(v, pltpu.HBM)
        for v in (out_grad, layer_input, expert_ids.T, gate_prob.T, scale_exps, w_stack)
    ))
    weight_grads, input_grad = pl.pallas_call(
        store_kernel,
        in_specs=[vm, vm],
        out_specs=(pl.BlockSpec(memory_space=pl.ANY), pl.BlockSpec(memory_space=pl.ANY)),
        out_shape=(
            jax.ShapeDtypeStruct((3, depth, hid), F32),
            jax.ShapeDtypeStruct((tok, width), BF),
        ),
        scratch_shapes=[dma((4,))],
        compiler_params=pltpu.CompilerParams(vmem_limit_bytes=VMEM_LIMIT),
    )(weight_grads, input_grad)
    return input_grad, weight_grads


def solution(mesh):
    in_specs = (
        P(("dp", "expert"), None),
        P(("dp", "expert"), None),
        P(("dp", "expert"), None),
        P(("dp", "expert"), None),
        P(None, "dp", "expert"),
        P(None, "dp", "expert"),
    )
    out_specs = (P(("dp", "expert"), None), P(None, "dp", "expert"))
    return jax.shard_map(
        functools.partial(per_device, mesh.shape["dp"], mesh.shape["expert"]),
        mesh=mesh, in_specs=in_specs, out_specs=out_specs, check_vma=False,
    )
```

```python
import functools

import jax
import jax.numpy as jnp
from jax import lax
from jax.experimental import pallas as pl
from jax.experimental.pallas import tpu as pltpu
from jax.sharding import PartitionSpec as P

TILE = 128
CAP = 3
DIRECT = 64
TALL = 256
BF = jnp.bfloat16
F32 = jnp.float32
VMEM_LIMIT = 40 * 1024 * 1024


def iota(shape, dim):
    return lax.broadcasted_iota(jnp.int32, shape, dim)


def mm(a, b, ca=1, cb=0):
    return lax.dot_general(a, b, (((ca,), (cb,)), ((), ())), preferred_element_type=F32)


def up8(n):
    return -(-n // 8) * 8


def step_to(i, k, n):
    return i ^ k if n & (n - 1) == 0 else lax.rem(i + k, n)


def steps_between(i, t, n):
    return i ^ t if n & (n - 1) == 0 else lax.rem(t - i + n, n)


def step_from(i, k, n):
    return i ^ k if n & (n - 1) == 0 else lax.rem(i - k + n, n)


def pad_rows(val, n):
    if val.shape[0] == n:
        return val
    return jnp.concatenate([val, jnp.zeros((n - val.shape[0], val.shape[1]), val.dtype)], axis=0)


class Batch:
    def __init__(self, steps, first, last, n_dp, hid):
        self.steps = steps
        self.rows = len(steps) * 2 * CAP
        self.padded = up8(self.rows)
        tight = up8(3 * self.rows) < 3 * self.padded
        self.stride = self.rows if tight else self.padded
        self.first = first
        self.last = last
        self.all = n_dp * self.padded
        self.local = first // n_dp
        self.sum_rows = up8(3 * self.stride)
        self.act_rows = up8(2 * self.stride)
        self.chunk = min(128, hid) if last else hid
        self.n_chunk = hid // self.chunk

    def cols(self, c):
        return slice(c * self.chunk, (c + 1) * self.chunk)


def plan_batches(n_dp, n_ex, hid):
    pairs = n_ex // 2
    groups = [[0], list(range(1, pairs))] if 1 < pairs <= 4 else [list(range(pairs))]
    batches, first = [], 0
    for i, steps in enumerate(groups):
        batches.append(Batch(steps, first, i == len(groups) - 1, n_dp, hid))
        first += batches[-1].all
        batches[-1].slot = sum(b.n_chunk for b in batches[:-1])
    return batches


def exchange_kernel(
    n_dp, n_ex, batches,
    og_hbm, li_hbm, ids_hbm, prob_hbm, exps_hbm, w_hbm,
    wg_ref, ig_ref, *scratch,
):
    n_b = len(batches)
    (
        og_ref, li_ref, ids_ref, prob_ref, exps_ref, xt, act, w, slab_out, slabs, x, hid_out, hid_in,
        acc, back_out, back_in, own_out, own_in,
        in_sem, s1_send, s1_recv, s2_send, s2_recv, s3_send, s3_recv, ready,
        rs_send, rs_recv, ag_send, ag_recv, hg_sem, b1_sem,
    ) = scratch[:32]
    if n_dp * n_ex > DIRECT:
        b2_sem = scratch[32]
    bufs = scratch[32 + (n_dp * n_ex > DIRECT):]
    part_out, part_in, act_out, act_in = (bufs[i * n_b:(i + 1) * n_b] for i in range(4))
    p, e = lax.axis_index("dp"), lax.axis_index("expert")
    tok, width = og_hbm.shape
    _, depth, hid = w.shape
    pairs = n_ex // 2
    z, core = e // 2, e % 2
    other = 1 - core
    partner = 2 * z + other

    def send(src, dst, ssem, rsem, q, f):
        pltpu.make_async_remote_copy(
            src_ref=src, dst_ref=dst, send_sem=ssem, recv_sem=rsem,
            device_id=(q, f), device_id_type=pl.DeviceIdType.MESH,
        ).start()

    def wait(ref, sem):
        pltpu.make_async_copy(ref, ref, sem).wait()

    def tell(sem, q, f):
        pl.semaphore_signal(sem, inc=1, device_id=(q, f), device_id_type=pl.DeviceIdType.MESH)

    in_copies = [
        pltpu.make_async_copy(src, dst, in_sem.at[i])
        for i, (src, dst) in enumerate((
            (ids_hbm, ids_ref), (prob_hbm, prob_ref), (li_hbm, li_ref),
            (og_hbm, og_ref), (exps_hbm, exps_ref),
            (w_hbm.at[0], w.at[0]), (w_hbm.at[1], w.at[1]), (w_hbm.at[2], w.at[2]),
        ))
    ]
    for copy in in_copies[:5]:
        copy.start()

    barrier = pltpu.get_barrier_semaphore()
    for k in range(1, n_dp):
        tell(barrier, step_from(p, k, n_dp), partner)
    tell(barrier, p, partner)
    for j in range(1, pairs):
        s = step_from(z, j, pairs)

        @pl.when(s > z)
        def _(s=s):
            tell(barrier, p, 2 * s + other)

    for copy in in_copies[:2]:
        copy.wait()
    routed = ids_ref[...] == 0
    mask = jnp.max(routed.astype(F32), axis=0, keepdims=True)
    prob = jnp.sum(jnp.where(routed, prob_ref[...], 0.0), axis=0, keepdims=True)
    earlier = (iota((tok, tok), 0) <= iota((tok, tok), 1)).astype(BF)
    place = mm(jnp.broadcast_to(mask, (8, tok)).astype(BF), earlier) - 1.0
    mask_tall = jnp.broadcast_to(mask, (8, tok)) > 0.5
    row = iota((8, tok), 0).astype(F32)
    hit_in = jnp.where((place == row) & (row < CAP) & mask_tall, 1.0, 0.0)
    hit_gr = jnp.where((place + CAP == row) & (row >= CAP) & mask_tall, 1.0, 0.0)
    row_prob = jnp.sum(hit_gr * prob, axis=1, keepdims=True)
    for copy in in_copies[2:4]:
        copy.wait()
    for copy in in_copies[5:]:
        copy.start()
    slots = (
        mm(hit_in.astype(BF), li_ref[...]) + row_prob * mm(hit_gr.astype(BF), og_ref[...])
    ).astype(BF)
    for q in range(n_dp):
        slab_out[q] = slots[:, q * depth:(q + 1) * depth]
    pl.semaphore_wait(barrier, n_dp + z)

    for k in range(n_dp - 1, 0, -1):
        q = step_to(p, k, n_dp)
        send(slab_out.at[q], slabs.at[z, other, p], s1_send, s1_recv.at[k - 1], q, partner)
    for j in range(1, pairs):
        s = step_from(z, j, pairs)

        @pl.when(s < z)
        def _(s=s, j=j):
            tell(ready.at[j - 1], p, 2 * s + other)

    slabs[z, core, p] = slab_out[p]

    def forward_down(src):
        for j in range(pairs - 1, 0, -1):
            t = step_to(z, j, pairs)

            @pl.when(t < z)
            def _(t=t, j=j):
                send(src, src, s2_send, s2_recv.at[j - 1], p, 2 * t + other)

    fine = n_dp <= 4
    if fine:
        forward_down(slabs.at[z, core, p])

    in_copies[4].wait()
    tr, tc = depth // TILE, hid // TILE

    def scale_rows(m, r, carry):
        at = pl.ds(pl.multiple_of(r * TILE, TILE), TILE)
        for j in range(tc):
            power = lax.shift_left(jnp.int32(1), exps_ref[m, r, j] + 15)
            factor = power.astype(F32) * (2.0 ** -15)
            cols = slice(j * TILE, (j + 1) * TILE)
            w[m, at, cols] = (w[m, at, cols].astype(F32) * factor).astype(BF)
        return carry

    for m in range(3):
        in_copies[5 + m].wait()
        lax.fori_loop(0, tr, functools.partial(scale_rows, m), 0)

    for k in range(1, n_dp):
        q = step_from(p, k, n_dp)
        wait(slabs.at[z, core, q], s1_recv.at[k - 1])
        if fine:
            forward_down(slabs.at[z, core, q])
    held = slabs.at[z, core]
    send(held, held, s3_send, s3_recv.at[0], p, partner)
    if not fine:
        forward_down(held)
    for j in range(1, pairs):
        t = step_to(z, j, pairs)

        @pl.when(t > z)
        def _(t=t, j=j):
            pl.semaphore_wait(ready.at[j - 1], 1)
            send(held, held, s2_send, s2_recv.at[j - 1], p, 2 * t + other)

    def pass_on(b):
        for j in b.steps:
            if j:
                block = slabs.at[step_from(z, j, pairs), other]
                wait(block, s2_recv.at[j - 1])
                send(block, block, s3_send, s3_recv.at[n_b - 1], p, partner)

    def collect(b):
        if not b.last:
            wait(slabs.at[z, other], s3_recv.at[0])
        else:
            wait(slabs.at[0:len(b.steps), 0], s3_recv.at[n_b - 1])
        shape = (2 * b.padded, len(b.steps) * 16)
        src, dst = iota(shape, 1), iota(shape, 0)
        kind, r = dst // b.padded, dst % b.padded
        jl, cs, c = r // (2 * CAP), (r // CAP) % 2, r % CAP
        rows = [[], []]
        for g in range(n_dp):
            h = jnp.where(g == p, cs, 1 - cs)
            pick = jnp.where(
                (src == jl * 16 + h * 8 + kind * CAP + c) & (r < b.rows), 1.0, 0.0
            ).astype(BF)
            have = jnp.concatenate(
                [slabs[step_from(z, j, pairs), :, g].reshape(16, depth) for j in b.steps], axis=0
            )
            val = mm(pick, have)
            for i in range(2):
                rows[i].append(val[i * b.padded:(i + 1) * b.padded])
        for i in range(2):
            x[i, b.first:b.first + b.all] = jnp.concatenate(rows[i], axis=0).astype(BF)

    def multiply(n, c):
        b = batches[n]
        vals = [
            mm(x[m // 2, b.first:b.first + b.all], w[m, :, b.cols(c)]) for m in range(3)
        ]
        for g in range(n_dp):
            at = g * b.padded
            block = jnp.concatenate([v[at:at + b.stride] for v in vals], axis=0)
            part_out[n][c, g] = pad_rows(block, b.sum_rows).astype(BF)
        for k in range(n_dp - 1, -1, -1):
            q = step_to(p, k, n_dp)
            send(part_out[n].at[c, q], part_in[n].at[c, p], rs_send.at[n], rs_recv.at[b.slot + c], q, partner)

    def activate(n, c):
        b = batches[n]
        wait(part_in[n].at[c], rs_recv.at[b.slot + c])
        total = part_in[n][c, 0].astype(F32)
        for g in range(1, n_dp):
            total = total + part_in[n][c, g].astype(F32)
        gate, up, down = (total[m * b.stride:(m + 1) * b.stride] for m in range(3))
        sig = jax.nn.sigmoid(gate)
        silu = gate * sig
        grads = [down * up * sig * (1.0 + gate * (1.0 - sig)), down * silu]
        hid_out[b.local:b.local + b.padded, b.cols(c)] = pad_rows(silu * up, b.padded).astype(BF)
        act_out[n][c] = pad_rows(jnp.concatenate(grads, axis=0), b.act_rows).astype(BF)
        for k in range(n_dp - 1, -1, -1):
            q = step_to(p, k, n_dp)
            send(
                act_out[n].at[c], act_in[n].at[c, p], ag_send.at[n], ag_recv.at[b.slot + c],
                q, partner,
            )

    if n_b == 1:
        pass_on(batches[0])
    collect(batches[0])
    if n_b > 1:
        multiply(0, 0)
        pass_on(batches[1])
        activate(0, 0)
        collect(batches[1])
    for c in range(batches[-1].n_chunk):
        multiply(n_b - 1, c)

    for i in range(2):
        xt[i] = x[i].astype(F32).T.astype(BF)

    for n, b in list(enumerate(batches))[-1:]:
        for c in range(b.n_chunk):
            activate(n, c)
    for k in range(n_dp - 1, -1, -1):
        send(hid_out, hid_in.at[p], hg_sem.at[0], hg_sem.at[1], step_to(p, k, n_dp), partner)

    def unpack(n, c):
        b = batches[n]
        wait(act_in[n].at[c], ag_recv.at[b.slot + c])
        blocks = [act_in[n][c, g].astype(F32) for g in range(n_dp)]
        for m in range(2):
            val = [pad_rows(v[m * b.stride:(m + 1) * b.stride], b.padded) for v in blocks]
            act[m, b.first:b.first + b.all, b.cols(c)] = jnp.concatenate(val, axis=0).astype(BF)

    for n, b in enumerate(batches):
        for c in range(b.n_chunk):
            unpack(n, c)
            if b.last:
                cols = b.cols(c)
                part = mm(act[0, :, cols], w[0, :, cols], 1, 1) + mm(act[1, :, cols], w[1, :, cols], 1, 1)
                if c == 0:
                    acc[...] = part
                else:
                    acc[...] += part

    pad = n_dp * 2
    half = depth // 2
    summed = acc[...].astype(BF)
    some = min(n_ex, 8)
    for i in range(n_ex // some):
        shape = (some * pad, summed.shape[0])
        to, frm = iota(shape, 0), iota(shape, 1)
        f, g = to // pad + i * some, (to % pad) // 2
        cs = jnp.where(core == 0, f % 2, 1 - f % 2)
        if n_b == 1:
            base = g * batches[0].padded + (f // 2) * 2 * CAP
        else:
            base = 0
            for b in batches:
                for jl, j in enumerate(b.steps):
                    base = jnp.where(f // 2 == j, b.first + g * b.padded + jl * 2 * CAP, base)
        base = base + cs * CAP
        parts = []
        for t in range(CAP):
            piece = CAP * (to % 2) + t
            val = 0.0
            for h in range(2):
                choose = jnp.where(
                    (piece % 2 == h) & (frm == base + piece // 2), 1.0, 0.0
                ).astype(BF)
                val = val + mm(choose, summed[:, h * half:(h + 1) * half])
            parts.append(val)
        val = jnp.concatenate(parts, axis=1)
        for j in range(some):
            for g in range(n_dp):
                at = j * pad + g * 2
                back_out[i * some + j, g] = val[at:at + 2].astype(BF)

    tall = min(TALL, depth)

    def weight_grads():
        for m in range(3):
            if m == 2:
                wait(hid_in, hg_sem.at[1])
                for b in batches:
                    act[2, b.first:b.first + b.all] = jnp.concatenate(
                        [hid_in[g, b.local:b.local + b.padded].astype(F32) for g in range(n_dp)],
                        axis=0,
                    ).astype(BF)
            for r in range(0, depth, tall):
                at = slice(r, r + tall)
                wg_ref[m, at, :] = mm(xt[m // 2, at, :], act[m])

    def place(q, packed):
        halves = [
            packed[j // CAP:j // CAP + 1, (j % CAP) * half:(j % CAP + 1) * half]
            for j in range(2 * CAP)
        ]
        back_rows = jnp.concatenate(
            [jnp.concatenate(halves[2 * c:2 * c + 2], axis=1) for c in range(CAP)], axis=0
        ).astype(BF)
        ig_ref[:, pl.ds(pl.multiple_of(q * depth, TILE), depth)] = mm(
            hit_in[:CAP].astype(BF), back_rows, 0, 0
        ).astype(BF)

    def far(k):
        return 2 * step_to(z, k // 2, pairs) + (core ^ (k % 2))

    if n_dp * n_ex <= DIRECT:
        def give(q, f):
            k = 2 * steps_between(z, f // 2, pairs) + (core ^ (f % 2))
            send(
                back_out.at[k, q], back_in.at[k * n_dp + steps_between(p, q, n_dp)],
                b1_sem.at[0], b1_sem.at[1], q, f,
            )

        for f in range(2):
            @pl.when((p > 0) | (e != f))
            def _(f=f):
                give(0, f)

        for r in range(n_ex * n_dp - 1, 0, -1):
            q, f = step_to(p, r % n_dp, n_dp), far(r // n_dp)

            @pl.when((q > 0) | (f > 1))
            def _(q=q, f=f):
                give(q, f)

        back_in[0] = back_out[0, p]
        weight_grads()
        arrived = back_in.at[1:n_ex * n_dp]
        wait(arrived, b1_sem.at[1])
        for k in range(n_dp):
            total = back_in[k].astype(F32)
            for f in range(1, n_ex):
                total = total + back_in[f * n_dp + k].astype(F32)
            place(step_from(p, k, n_dp), total)
        wait(arrived, b1_sem.at[0])
    else:
        for k in range(1, n_ex):
            send(back_out.at[k], back_in.at[k], b1_sem.at[0], b1_sem.at[1], p, far(k))
        weight_grads()
        arrived = back_in.at[1:n_ex]
        wait(arrived, b1_sem.at[1])
        for g in range(n_dp):
            total = back_out[0, g].astype(F32)
            for k in range(1, n_ex):
                total = total + back_in[k, g].astype(F32)
            own_out[g] = total.astype(BF)
        for k in range(1, n_dp):
            q = step_to(p, k, n_dp)
            send(own_out.at[q], own_in.at[k], b2_sem.at[0], b2_sem.at[1], q, e)
        own_in[0] = own_out[p]
        landed = own_in.at[1:n_dp]
        wait(landed, b2_sem.at[1])
        for k in range(n_dp):
            place(step_from(p, k, n_dp), own_in[k].astype(F32))
        wait(arrived, b1_sem.at[0])
        wait(landed, b2_sem.at[0])

    wait(slab_out.at[1:n_dp], s1_send)
    wait(slabs.at[1:pairs, 0], s2_send)
    wait(slabs.at[:, 0], s3_send)
    for n in range(n_b):
        wait(part_out[n], rs_send.at[n])
        wait(act_in[n], ag_send.at[n])
    wait(hid_in, hg_sem.at[0])


def store_kernel(wg_ref, ig_ref, wg_hbm, ig_hbm, sems):
    copies = [pltpu.make_async_copy(ig_ref, ig_hbm, sems.at[3])]
    for m in range(3):
        copies.append(pltpu.make_async_copy(wg_ref.at[m], wg_hbm.at[m], sems.at[m]))
    for copy in copies:
        copy.start()
    for copy in copies:
        copy.wait()


def per_device(n_dp, n_ex, out_grad, layer_input, expert_ids, gate_prob, w_stack, scale_exps):
    tok, width = out_grad.shape
    _, depth, hid = w_stack.shape
    batches = plan_batches(n_dp, n_ex, hid)
    total = sum(b.all for b in batches)
    n_b = len(batches)
    parts = sum(b.n_chunk for b in batches)
    pairs = n_ex // 2
    packed = (2, CAP * depth // 2)
    direct = n_dp * n_ex <= DIRECT
    vm = pl.BlockSpec(memory_space=pltpu.VMEM)
    dma = pltpu.SemaphoreType.DMA
    weight_grads, input_grad = pl.pallas_call(
        functools.partial(exchange_kernel, n_dp, n_ex, batches),
        out_shape=(
            jax.ShapeDtypeStruct((3, depth, hid), F32),
            jax.ShapeDtypeStruct((tok, width), BF),
        ),
        in_specs=[pl.BlockSpec(memory_space=pltpu.HBM)] * 6,
        out_specs=(vm, vm),
        scratch_shapes=[
            pltpu.VMEM((tok, width), BF),
            pltpu.VMEM((tok, width), BF),
            pltpu.VMEM((2, tok), jnp.int32),
            pltpu.VMEM((2, tok), F32),
            pltpu.SMEM(scale_exps.shape, jnp.int32),
            pltpu.VMEM((2, depth, total), BF),
            pltpu.VMEM((3, total, hid), BF),
            pltpu.VMEM((3, depth, hid), BF),
            pltpu.VMEM((n_dp, 8, depth), BF),
            pltpu.VMEM((pairs, 2, n_dp, 8, depth), BF),
            pltpu.VMEM((2, total, depth), BF),
            pltpu.VMEM((total // n_dp, hid), BF),
            pltpu.VMEM((n_dp, total // n_dp, hid), BF),
            pltpu.VMEM((total, depth), F32),
            pltpu.VMEM((n_ex, n_dp) + packed, BF),
            pltpu.VMEM(((n_ex * n_dp,) if direct else (n_ex, n_dp)) + packed, BF),
            pltpu.VMEM((n_dp,) + packed, BF),
            pltpu.VMEM((n_dp,) + packed, BF),
            dma((8,)),
            dma, dma((n_dp - 1,)),
            dma, dma((pairs - 1,)),
            dma, dma((n_b,)),
            pltpu.SemaphoreType.REGULAR((pairs - 1,)),
            dma((n_b,)), dma((parts,)),
            dma((n_b,)), dma((parts,)),
            dma((2,)), dma((2,))] + [dma((2,))] * (not direct) + [
        ]
        + [pltpu.VMEM((b.n_chunk, n_dp, b.sum_rows, b.chunk), BF) for b in batches]
        + [pltpu.VMEM((b.n_chunk, n_dp, b.sum_rows, b.chunk), BF) for b in batches]
        + [pltpu.VMEM((b.n_chunk, b.act_rows, b.chunk), BF) for b in batches]
        + [pltpu.VMEM((b.n_chunk, n_dp, b.act_rows, b.chunk), BF) for b in batches],
        compiler_params=pltpu.CompilerParams(
            collective_id=0, has_side_effects=True, vmem_limit_bytes=VMEM_LIMIT
        ),
    )(*(
        pltpu.with_memory_space_constraint(v, pltpu.HBM)
        for v in (out_grad, layer_input, expert_ids.T, gate_prob.T, scale_exps, w_stack)
    ))
    weight_grads, input_grad = pl.pallas_call(
        store_kernel,
        in_specs=[vm, vm],
        out_specs=(pl.BlockSpec(memory_space=pl.ANY), pl.BlockSpec(memory_space=pl.ANY)),
        out_shape=(
            jax.ShapeDtypeStruct((3, depth, hid), F32),
            jax.ShapeDtypeStruct((tok, width), BF),
        ),
        scratch_shapes=[dma((4,))],
        compiler_params=pltpu.CompilerParams(vmem_limit_bytes=VMEM_LIMIT),
    )(weight_grads, input_grad)
    return input_grad, weight_grads


def solution(mesh):
    in_specs = (
        P(("dp", "expert"), None),
        P(("dp", "expert"), None),
        P(("dp", "expert"), None),
        P(("dp", "expert"), None),
        P(None, "dp", "expert"),
        P(None, "dp", "expert"),
    )
    out_specs = (P(("dp", "expert"), None), P(None, "dp", "expert"))
    return jax.shard_map(
        functools.partial(per_device, mesh.shape["dp"], mesh.shape["expert"]),
        mesh=mesh, in_specs=in_specs, out_specs=out_specs, check_vma=False,
    )
```
